16 devices in a mesh: tp: 4 (over z, y), dp: 4 (over x, core).
Axes of the slice: x: 2, y: 2, z: 2, core: 2. Of those that a mesh axis runs over, the one named last changes fastest.
Arguments:
- x: bfloat16 [512, 2048], P('dp')
- lengths: int32 [512], P('dp')
- cache: bfloat16 [2, 512, 512, 576], P(None, 'dp')
- attn_norm: bfloat16 [2, 2048], replicated
- ffn_norm: bfloat16 [2, 2048], replicated
- wq: bfloat16 [2, 2048, 9216], P(None, None, 'tp')
- wo: bfloat16 [2, 8192, 2048], P(None, 'tp')
- w1: bfloat16 [2, 2048, 10944], P(None, None, ('dp', 'tp'))
- w3: bfloat16 [2, 2048, 10944], P(None, None, ('dp', 'tp'))
- w2: bfloat16 [2, 10944, 2048], P(None, ('dp', 'tp'))
Outputs:
- output: bfloat16 [512, 2048], P('dp')
All inputs are finite; a program needn't handle non-finite values.
Results may differ from the reference program's by a relative error of at most 0.02.
Values are sent between devices in bfloat16 or wider.
A program may use at most 1 GiB of HBM per device.

```python
import jax
import jax.numpy as jnp
from jax import lax

B = 512
S = 512
D = 2048
H = 16
F = 10944
LAYERS = 2
LAT = 512
ROPE = 64
KV = LAT + ROPE
EPS = 1e-6
SCALE = 192 ** -0.5


def setup_inputs(seed: int = 0) -> dict:
    ks = jax.random.split(jax.random.PRNGKey(seed), 10)

    def nrm(k, shape, std):
        return (jax.random.normal(k, shape, jnp.float32) * std).astype(jnp.bfloat16)

    def gain(k):
        return jax.random.uniform(k, (LAYERS, D), jnp.float32, 0.5, 1.5).astype(jnp.bfloat16)

    return {
        'x': nrm(ks[0], (B, D), 1.0),
        'lengths': jax.random.randint(ks[1], (B,), max(S // 8, 1), S + 1, jnp.int32),
        'cache': nrm(ks[2], (LAYERS, B, S, KV), 1.0),
        'attn_norm': gain(ks[3]),
        'ffn_norm': gain(ks[4]),
        'wq': nrm(ks[5], (LAYERS, D, H * KV), D ** -0.5),
        'wo': nrm(ks[6], (LAYERS, H * LAT, D), (H * LAT) ** -0.5 * S ** 0.5 / 8),
        'w1': nrm(ks[7], (LAYERS, D, F), D ** -0.5),
        'w3': nrm(ks[8], (LAYERS, D, F), D ** -0.5),
        'w2': nrm(ks[9], (LAYERS, F, D), 2.0 * F ** -0.5),
    }


def _rmsnorm(v, w):
    vf = v.astype(jnp.float32)
    r = lax.rsqrt(jnp.mean(vf * vf, axis=-1, keepdims=True) + EPS)
    return (vf * r * w.astype(jnp.float32)).astype(jnp.bfloat16)


def _attend(q, c, n):
    s = jnp.dot(q, c.T, preferred_element_type=jnp.float32) * SCALE
    s = jnp.where(jnp.arange(c.shape[0])[None, :] < n, s, -jnp.inf)
    p = jax.nn.softmax(s, axis=-1).astype(jnp.bfloat16)
    return jnp.dot(p, c[:, :LAT], preferred_element_type=jnp.float32).astype(jnp.bfloat16)


def _layer(x, lengths, c, an, fn, wq, wo, w1, w3, w2):
    nb = x.shape[0]
    h = _rmsnorm(x, an)
    q = jnp.dot(h, wq, preferred_element_type=jnp.float32).astype(jnp.bfloat16).reshape(nb, H, KV)
    o = lax.map(lambda t: _attend(*t), (q, c, lengths)).reshape(nb, H * LAT)
    x = x + jnp.dot(o, wo, preferred_element_type=jnp.float32).astype(jnp.bfloat16)
    g = _rmsnorm(x, fn)
    u = jnp.dot(g, w3, preferred_element_type=jnp.float32)
    v = jnp.dot(g, w1, preferred_element_type=jnp.float32)
    a = (jax.nn.silu(u) * v).astype(jnp.bfloat16)
    return x + jnp.dot(a, w2, preferred_element_type=jnp.float32).astype(jnp.bfloat16)


def reference(x, lengths, cache, attn_norm, ffn_norm, wq, wo, w1, w3, w2):
    def body(xc, lw):
        return _layer(xc, lengths, *lw), None
    out, _ = lax.scan(body, x, (cache, attn_norm, ffn_norm, wq, wo, w1, w3, w2))
    return out
```

```python
import functools

import jax
import jax.numpy as jnp
from jax import lax
from jax.experimental import pallas as pl
from jax.experimental.pallas import tpu as pltpu
from jax.sharding import PartitionSpec as P

MESH = pl.DeviceIdType.MESH
F32 = jnp.float32
BF16 = jnp.bfloat16
LAT = 512
EPS = 1e-6
SCALE = 192 ** -0.5
VMEM_LIMIT = 64 * 1024 * 1024 - 65536 - 1024 * 1024

TP_ORDERS = (('z', 'y'), ('y', 'z'), ('z', 'y'), ('y', 'z'))
CUBE_ORDERS = (
    ('x', 'y', 'z'), ('y', 'z', 'x'), ('z', 'x', 'y'),
    ('x', 'y', 'z'), ('y', 'z', 'x'), ('z', 'x', 'y'),
    ('x', 'y', 'z'), ('y', 'z', 'x'),
)
RING = ((1, 0, 0), (0, 1, 0), (0, 0, 1), (0, 1, 1), (1, 1, 0), (1, 0, 1), (1, 1, 1))
TP_PEERS = ((1, 0), (0, 1), (1, 1))


class Place:
    def __init__(self):
        self.tp, self.dp = lax.axis_index('tp'), lax.axis_index('dp')
        self.z, self.y = lax.div(self.tp, 2), lax.rem(self.tp, 2)
        self.x, self.c = lax.div(self.dp, 2), lax.rem(self.dp, 2)
        self.at = {'x': self.x, 'z': self.z, 'y': self.y}

    def other(self, dx=0, dz=0, dy=0, dc=0):
        x = 1 - self.x if dx else self.x
        z = 1 - self.z if dz else self.z
        y = 1 - self.y if dy else self.y
        c = 1 - self.c if dc else self.c
        return {'tp': 2 * z + y, 'dp': 2 * x + c}

    def along(self, axis):
        return self.other(**{'d' + axis: 1})


def _send(src, dst, sems, k, device):
    copy = pltpu.make_async_remote_copy(
        src_ref=src, dst_ref=dst, send_sem=sems.at[0, k], recv_sem=sems.at[1, k],
        device_id=device, device_id_type=MESH,
    )
    copy.start()
    return copy


def _norm(v, w):
    vf = v.astype(F32)
    r = lax.rsqrt(jnp.mean(vf * vf, axis=-1, keepdims=True) + EPS)
    return (vf * r * w.astype(F32)).astype(BF16)


def _greet(devices):
    barrier = pltpu.get_barrier_semaphore()
    for device in devices:
        pl.semaphore_signal(barrier, inc=1, device_id=device, device_id_type=MESH)
    pl.semaphore_wait(barrier, len(devices))


class Halving:
    def __init__(self, here, axes, buf, recvs, sems, orders):
        self.here, self.axes, self.buf, self.recvs, self.sems, self.orders = here, axes, buf, recvs, sems, orders
        self.copies = {}

    def _view(self, chunk, phase, flip):
        index = [slice(None)] * len(self.axes)
        for p, axis in enumerate(self.orders[chunk][: phase + 1]):
            mine = self.here.at[axis]
            index[self.axes.index(axis)] = 1 - mine if (flip and p == phase) else mine
        return (chunk, *index)

    def send(self, chunk, phase):
        axis = self.orders[chunk][phase]
        self.copies[chunk, phase] = _send(
            self.buf.at[self._view(chunk, phase, True)], self.recvs[phase].at[chunk],
            self.sems, phase * len(self.orders) + chunk, self.here.along(axis),
        )

    def add(self, chunk, phase):
        self.copies[chunk, phase].wait_recv()
        view = self._view(chunk, phase, False)
        total = self.buf[view] + self.recvs[phase][chunk]
        if phase + 1 < len(self.axes):
            self.buf[view] = total
        return total

    def finish(self):
        for copy in self.copies.values():
            copy.wait_send()


def _q_exchange(here, h, wq_buf, wq_copies, q_send, q_recv, q_out, sems, width=768):
    copies = []
    cols = q_send.shape[-1]
    for n in range(cols // width):
        wq_copies[n].wait()
        part = slice(n * width, (n + 1) * width)
        q = jnp.dot(h, wq_buf[:, part], preferred_element_type=F32).astype(BF16)
        q_send[:, :, part] = q.reshape(4, -1, width)
        for k, (dz, dy) in enumerate(TP_PEERS):
            peer = here.other(dz=dz, dy=dy)
            copies.append(_send(
                q_send.at[peer['tp'], :, part], q_recv.at[here.tp, :, part], sems, 3 * n + k, peer,
            ))
    q_out[here.tp] = q_send[here.tp]
    for copy in copies:
        copy.wait_recv()
    for dz, dy in TP_PEERS:
        peer = here.other(dz=dz, dy=dy)
        q_out[peer['tp']] = q_recv[peer['tp']]
    for copy in copies:
        copy.wait_send()


def _wq_start(layer, wq_hbm, wq_buf, sems, width=768):
    copies = []
    for n in range(wq_buf.shape[1] // width):
        part = slice(n * width, (n + 1) * width)
        copies.append(pltpu.make_async_copy(wq_hbm.at[layer, :, part], wq_buf.at[:, part], sems.at[n]))
        copies[-1].start()
    return copies


def _first_kernel(x_ref, an_ref, wq_hbm, q_out, wq_buf, q_send, q_recv, wq_sems, q_sems):
    here = Place()
    wq_copies = _wq_start(0, wq_hbm, wq_buf, wq_sems)
    _greet([here.other(dz=dz, dy=dy) for dz, dy in TP_PEERS])
    h = _norm(x_ref[...], an_ref[0:1, :])
    _q_exchange(here, h, wq_buf, wq_copies, q_send, q_recv, q_out, q_sems)


def _attention_kernel(layer, len_ref, q_ref, cache_hbm, o_ref, c_buf, sems):
    depth, s_len, kv = c_buf.shape
    rows = q_ref.shape[0]
    block = 128
    blocks = s_len // block
    base = lax.axis_index('tp') * rows

    def length(b):
        return len_ref[base + b]

    def count(b):
        return lax.div(length(b) + (block - 1), block)

    def copy(b, j):
        slot = lax.rem(b, depth)
        part = pl.ds(j * block, block)
        return pltpu.make_async_copy(
            cache_hbm.at[layer, base + b, part, :], c_buf.at[slot, part, :], sems.at[slot, j]
        )

    def each(b, act):
        n = count(b)
        for j in range(blocks):
            @pl.when(j < n)
            def _():
                act(copy(b, j))

    c_buf[...] = jnp.zeros_like(c_buf)
    for b in range(depth - 2):
        each(b, lambda c: c.start())

    def attend(b, t):
        slot = lax.rem(b, depth)
        q = q_ref[b]
        s = lax.dot_general(
            q, c_buf[slot, 0:t, :], (((1,), (1,)), ((), ())), preferred_element_type=F32
        ) * SCALE
        keep = lax.broadcasted_iota(jnp.int32, s.shape, 1) < length(b)
        s = jnp.where(keep, s, -jnp.inf)
        e = jnp.exp(s - jnp.max(s, axis=-1, keepdims=True))
        p = (e / jnp.sum(e, axis=-1, keepdims=True)).astype(BF16)
        o = jnp.dot(p, c_buf[slot, 0:t, 0:LAT], preferred_element_type=F32)
        o_ref[b] = o.astype(BF16)

    @pl.loop(0, rows // 2)
    def _(i):
        b = 2 * i
        for k in range(2):
            @pl.when(b + depth - 2 + k < rows)
            def _():
                each(b + depth - 2 + k, lambda c: c.start())
        for k in range(2):
            each(b + k, lambda c: c.wait())
        n = jnp.maximum(count(b), count(b + 1))
        for m in range(1, blocks + 1):
            @pl.when(n == m)
            def _():
                attend(b, m * block)
                attend(b + 1, m * block)


def _layer_kernel(layer, last, o_ref, x_ref, an_ref, fn_ref, wo_hbm, w1_hbm, w3_hbm, w2_hbm, wq_hbm, *rest):
    outs, scratch = rest[: 1 if last else 2], rest[1 if last else 2:]
    (wo_buf, w1_buf, w3_buf, w2_buf, o_all, p_buf, pr1, pr2, g_all, a_buf, y_buf, yr1, yr2, yr3, x_buf, h_all,
     w_sems, ws_sems, o_sems, p_sems, g_sems, y_sems, h_sems, *more) = scratch
    here = Place()
    wo_copy = pltpu.make_async_copy(wo_hbm.at[layer], wo_buf, w_sems.at[0])
    wo_copy.start()
    own = [
        pltpu.make_async_copy(hbm.at[layer], buf.at[here.c], w_sems.at[1 + k])
        for k, (hbm, buf) in enumerate(((w3_hbm, w3_buf), (w1_hbm, w1_buf), (w2_hbm, w2_buf)))
    ]
    cube = [here.other(dx=dx, dz=dz, dy=dy) for dx, dz, dy in RING]
    partner = here.other(dc=1)
    _greet(cube + [partner])

    o_copies = []
    for k, (dz, dy) in enumerate(TP_PEERS):
        peer = here.other(dz=dz, dy=dy)
        o_copies.append(_send(o_ref.at[peer['tp']], o_all.at[here.tp], o_sems, k, peer))
    for copy in own:
        copy.start()
    swaps = [
        _send(hbm.at[layer], buf.at[here.c], ws_sems, k, partner)
        for k, (hbm, buf) in enumerate(((w3_hbm, w3_buf), (w1_hbm, w1_buf), (w2_hbm, w2_buf)))
    ]
    if not last:
        wq_buf, q_send, q_recv, wq_sems, q_sems = more
        wq_copies = _wq_start(layer + 1, wq_hbm, wq_buf, wq_sems)
    o_all[here.tp] = o_ref[here.tp]
    for copy in o_copies:
        copy.wait_recv()
    wo_copy.wait()

    heads, width = o_all.shape[1], p_buf.shape[-1]
    lhs = jnp.concatenate([o_all[:, h].reshape(-1, LAT) for h in range(heads)], axis=1)
    attn = Halving(here, ('z', 'y'), p_buf, (pr1, pr2), p_sems, TP_ORDERS)
    for n in range(len(TP_ORDERS)):
        part = slice(n * width, (n + 1) * width)
        p_buf[n] = jnp.dot(lhs, wo_buf[:, part], preferred_element_type=F32).reshape(p_buf.shape[1:])
        attn.send(n, 0)
    for n in range(len(TP_ORDERS)):
        attn.add(n, 0)
        attn.send(n, 1)
    x_mine = x_ref[here.tp] if layer == 0 else x_ref[...]
    for n in range(len(TP_ORDERS)):
        part = slice(n * width, (n + 1) * width)
        total = attn.add(n, 1).astype(BF16)
        x_buf[:, part] = (x_mine[:, part].astype(F32) + total.astype(F32)).astype(BF16)
    x_mid = x_buf[...]

    g_all[here.x, here.tp] = _norm(x_mid, fn_ref[layer:layer + 1, :])
    mine = g_all.at[here.x, here.tp]
    g_copies = [_send(mine, mine, g_sems, k, device) for k, device in enumerate(cube)]
    for copy in own:
        copy.wait()
    for copy in swaps:
        copy.wait_recv()
    for copy in g_copies:
        copy.wait_recv()

    g = g_all[...].reshape(-1, g_all.shape[-1])
    cols = w1_buf.shape[-1]

    @pl.loop(0, 2)
    def _(s):
        for lo in range(0, cols, 256):
            part = slice(lo, min(lo + 256, cols))
            u = jnp.dot(g, w3_buf[s, :, part], preferred_element_type=F32)
            v = jnp.dot(g, w1_buf[s, :, part], preferred_element_type=F32)
            a_buf[s, :, part] = (u * jax.nn.sigmoid(u) * v).astype(BF16)

    ffn = Halving(here, ('x', 'z', 'y'), y_buf, (yr1, yr2, yr3), y_sems, CUBE_ORDERS)
    width = y_buf.shape[-1]
    for n in range(len(CUBE_ORDERS)):
        part = slice(n * width, (n + 1) * width)
        y = jnp.dot(a_buf[0], w2_buf[0, :, part], preferred_element_type=F32)
        y += jnp.dot(a_buf[1], w2_buf[1, :, part], preferred_element_type=F32)
        y_buf[n] = y.reshape(y_buf.shape[1:])
        ffn.send(n, 0)
    for phase in range(2):
        for n in range(len(CUBE_ORDERS)):
            ffn.add(n, phase)
            ffn.send(n, phase + 1)
    for n in range(len(CUBE_ORDERS)):
        part = slice(n * width, (n + 1) * width)
        total = ffn.add(n, 2).astype(BF16)
        x_buf[:, part] = (x_mid[:, part].astype(F32) + total.astype(F32)).astype(BF16)
    x_new = x_buf[...]

    h_all[here.tp] = x_new if last else _norm(x_new, an_ref[layer + 1:layer + 2, :])
    mine = h_all.at[here.tp]
    h_copies = [
        _send(mine, mine, h_sems, k, here.other(dz=dz, dy=dy)) for k, (dz, dy) in enumerate(TP_PEERS)
    ]
    for copy in h_copies:
        copy.wait_recv()
    if last:
        outs[0][...] = h_all[...]
    else:
        outs[1][...] = x_new
        h = h_all[...].reshape(-1, h_all.shape[-1])
        _q_exchange(here, h, wq_buf, wq_copies, q_send, q_recv, outs[0], q_sems)
    attn.finish()
    ffn.finish()
    for copy in o_copies + swaps + g_copies + h_copies:
        copy.wait_send()


VM = pl.BlockSpec(memory_space=pltpu.VMEM)
ANY = pl.BlockSpec(memory_space=pl.ANY)
DMA = pltpu.SemaphoreType.DMA


def solution(mesh):
    def body(x, lengths, cache, attn_norm, ffn_norm, wq, wo, w1, w3, w2):
        nb, d = x.shape
        n_layers, _, s_len, kv = cache.shape
        heads = wq.shape[2] // kv
        rows = nb // 4
        cols = w1.shape[2]
        q_shape = (4, rows, heads * kv)

        def params(cid):
            return pltpu.CompilerParams(collective_id=cid, has_side_effects=True, vmem_limit_bytes=VMEM_LIMIT)

        q_scratch = [
            pltpu.VMEM((d, heads * kv), BF16),
            pltpu.VMEM(q_shape, BF16),
            pltpu.VMEM(q_shape, BF16),
            DMA((3,)),
            DMA((2, 9)),
        ]

        q = pl.pallas_call(
            _first_kernel,
            out_shape=jax.ShapeDtypeStruct(q_shape, BF16),
            in_specs=[VM, VM, ANY],
            out_specs=VM,
            scratch_shapes=q_scratch,
            compiler_params=params(0),
            name='q_first',
        )(x, attn_norm, wq)

        x_in = x.reshape(4, rows, d)
        for layer in range(n_layers):
            last = layer == n_layers - 1
            qt = q.reshape(4, rows, heads, kv).transpose(1, 0, 2, 3).reshape(rows, 4 * heads, kv)
            o = pl.pallas_call(
                functools.partial(_attention_kernel, layer),
                out_shape=jax.ShapeDtypeStruct((rows, 4 * heads, LAT), BF16),
                in_specs=[pl.BlockSpec(memory_space=pltpu.SMEM), VM, ANY],
                out_specs=VM,
                scratch_shapes=[pltpu.VMEM((8, s_len, kv), BF16), DMA((8, s_len // 128))],
                compiler_params=pltpu.CompilerParams(vmem_limit_bytes=VMEM_LIMIT),
                name='attention',
            )(lengths, qt, cache)
            ot = o.reshape(rows, 4, heads, LAT).transpose(1, 2, 0, 3)
            scratch = [
                pltpu.VMEM(wo.shape[1:], BF16),
                pltpu.VMEM((2, d, cols), BF16),
                pltpu.VMEM((2, d, cols), BF16),
                pltpu.VMEM((2, cols, d), BF16),
                pltpu.VMEM((4, heads, rows, LAT), BF16),
                pltpu.VMEM((4, 2, 2, rows, d // 4), F32),
                pltpu.VMEM((4, 2, rows, d // 4), F32),
                pltpu.VMEM((4, rows, d // 4), F32),
                pltpu.VMEM((2, 4, rows, d), BF16),
                pltpu.VMEM((2, 8 * rows, cols), BF16),
                pltpu.VMEM((8, 2, 2, 2, rows, d // 8), F32),
                pltpu.VMEM((8, 2, 2, rows, d // 8), F32),
                pltpu.VMEM((8, 2, rows, d // 8), F32),
                pltpu.VMEM((8, rows, d // 8), F32),
                pltpu.VMEM((rows, d), BF16),
                pltpu.VMEM((4, rows, d), BF16),
                DMA((4,)),
                DMA((2, 3)),
                DMA((2, 3)),
                DMA((2, 8)),
                DMA((2, 7)),
                DMA((2, 24)),
                DMA((2, 3)),
            ]
            if last:
                out_shape = [jax.ShapeDtypeStruct((4, rows, d), BF16)]
            else:
                out_shape = [jax.ShapeDtypeStruct(q_shape, BF16), jax.ShapeDtypeStruct((rows, d), BF16)]
                scratch += q_scratch
            outs = pl.pallas_call(
                functools.partial(_layer_kernel, layer, last),
                out_shape=out_shape,
                in_specs=[VM, VM, VM, VM, ANY, ANY, ANY, ANY, ANY],
                out_specs=[VM] * len(out_shape),
                scratch_shapes=scratch,
                compiler_params=params(1 + layer),
                name=f'layer_{layer}',
            )(ot, x_in, attn_norm, ffn_norm, wo, w1, w3, w2, wq)
            if last:
                return outs[0].reshape(nb, d)
            q, x_in = outs

    in_specs = (
        P('dp', None),
        P('dp'),
        P(None, 'dp', None, None),
        P(None, None),
        P(None, None),
        P(None, None, 'tp'),
        P(None, 'tp', None),
        P(None, None, ('dp', 'tp')),
        P(None, None, ('dp', 'tp')),
        P(None, ('dp', 'tp'), None),
    )
    return jax.shard_map(body, mesh=mesh, in_specs=in_specs, out_specs=P('dp', None), check_vma=False)
```

```python
import functools

import jax
import jax.numpy as jnp
from jax import lax
from jax.experimental import pallas as pl
from jax.experimental.pallas import tpu as pltpu
from jax.sharding import PartitionSpec as P

MESH = pl.DeviceIdType.MESH
F32 = jnp.float32
BF16 = jnp.bfloat16
LAT = 512
EPS = 1e-6
SCALE = 192 ** -0.5
VMEM_LIMIT = 64 * 1024 * 1024 - 65536 - 1024 * 1024

TP_ORDERS = (('z', 'y'), ('y', 'z'), ('z', 'y'), ('y', 'z'))
CUBE_ORDERS = (
    ('x', 'y', 'z'), ('y', 'z', 'x'), ('z', 'x', 'y'),
    ('x', 'y', 'z'), ('y', 'z', 'x'), ('z', 'x', 'y'),
    ('x', 'y', 'z'), ('y', 'z', 'x'),
)
RING = ((1, 0, 0), (0, 1, 0), (0, 0, 1), (0, 1, 1), (1, 1, 0), (1, 0, 1), (1, 1, 1))
TP_PEERS = ((1, 0), (0, 1), (1, 1))


class Place:
    def __init__(self):
        self.tp, self.dp = lax.axis_index('tp'), lax.axis_index('dp')
        self.z, self.y = lax.div(self.tp, 2), lax.rem(self.tp, 2)
        self.x, self.c = lax.div(self.dp, 2), lax.rem(self.dp, 2)
        self.at = {'x': self.x, 'z': self.z, 'y': self.y}

    def other(self, dx=0, dz=0, dy=0, dc=0):
        x = 1 - self.x if dx else self.x
        z = 1 - self.z if dz else self.z
        y = 1 - self.y if dy else self.y
        c = 1 - self.c if dc else self.c
        return {'tp': 2 * z + y, 'dp': 2 * x + c}

    def along(self, axis):
        return self.other(**{'d' + axis: 1})


def _send(src, dst, sems, k, device):
    copy = pltpu.make_async_remote_copy(
        src_ref=src, dst_ref=dst, send_sem=sems.at[0, k], recv_sem=sems.at[1, k],
        device_id=device, device_id_type=MESH,
    )
    copy.start()
    return copy


def _norm(v, w):
    vf = v.astype(F32)
    r = lax.rsqrt(jnp.mean(vf * vf, axis=-1, keepdims=True) + EPS)
    return (vf * r * w.astype(F32)).astype(BF16)


def _greet(devices):
    barrier = pltpu.get_barrier_semaphore()
    for device in devices:
        pl.semaphore_signal(barrier, inc=1, device_id=device, device_id_type=MESH)
    pl.semaphore_wait(barrier, len(devices))


class Halving:
    def __init__(self, here, axes, buf, recvs, sems, orders):
        self.here, self.axes, self.buf, self.recvs, self.sems, self.orders = here, axes, buf, recvs, sems, orders
        self.copies = {}

    def _view(self, chunk, phase, flip):
        index = [slice(None)] * len(self.axes)
        for p, axis in enumerate(self.orders[chunk][: phase + 1]):
            mine = self.here.at[axis]
            index[self.axes.index(axis)] = 1 - mine if (flip and p == phase) else mine
        return (chunk, *index)

    def send(self, chunk, phase):
        axis = self.orders[chunk][phase]
        self.copies[chunk, phase] = _send(
            self.buf.at[self._view(chunk, phase, True)], self.recvs[phase].at[chunk],
            self.sems, phase * len(self.orders) + chunk, self.here.along(axis),
        )

    def add(self, chunk, phase):
        self.copies[chunk, phase].wait_recv()
        view = self._view(chunk, phase, False)
        total = self.buf[view] + self.recvs[phase][chunk]
        if phase + 1 < len(self.axes):
            self.buf[view] = total
        return total

    def finish(self):
        for copy in self.copies.values():
            copy.wait_send()


def _q_exchange(here, h, wq_buf, wq_copies, q_send, q_recv, q_out, sems, width=768):
    copies = []
    cols = q_send.shape[-1]
    for n in range(cols // width):
        wq_copies[n].wait()
        part = slice(n * width, (n + 1) * width)
        q = jnp.dot(h, wq_buf[:, part], preferred_element_type=F32).astype(BF16)
        q_send[:, :, part] = q.reshape(4, -1, width)
        for k, (dz, dy) in enumerate(TP_PEERS):
            peer = here.other(dz=dz, dy=dy)
            copies.append(_send(
                q_send.at[peer['tp'], :, part], q_recv.at[here.tp, :, part], sems, 3 * n + k, peer,
            ))
    q_out[here.tp] = q_send[here.tp]
    for copy in copies:
        copy.wait_recv()
    for dz, dy in TP_PEERS:
        peer = here.other(dz=dz, dy=dy)
        q_out[peer['tp']] = q_recv[peer['tp']]
    for copy in copies:
        copy.wait_send()


def _wq_start(layer, wq_hbm, wq_buf, sems, width=768):
    copies = []
    for n in range(wq_buf.shape[1] // width):
        part = slice(n * width, (n + 1) * width)
        copies.append(pltpu.make_async_copy(wq_hbm.at[layer, :, part], wq_buf.at[:, part], sems.at[n]))
        copies[-1].start()
    return copies


def _first_kernel(x_ref, an_ref, wq_hbm, q_out, wq_buf, q_send, q_recv, wq_sems, q_sems):
    here = Place()
    wq_copies = _wq_start(0, wq_hbm, wq_buf, wq_sems)
    _greet([here.other(dz=dz, dy=dy) for dz, dy in TP_PEERS])
    h = _norm(x_ref[...], an_ref[0:1, :])
    _q_exchange(here, h, wq_buf, wq_copies, q_send, q_recv, q_out, q_sems)


def _attention_kernel(layer, len_ref, q_ref, cache_hbm, o_ref, c_buf, sems):
    depth, kv, s_len = c_buf.shape
    rows = q_ref.shape[0]
    block = 128
    blocks = s_len // block
    base = lax.axis_index('tp') * rows

    def length(b):
        return len_ref[base + b]

    def count(b):
        return lax.div(length(b) + (block - 1), block)

    def copy(b, j):
        slot = lax.rem(b, depth)
        part = pl.ds(j * block, block)
        return pltpu.make_async_copy(
            cache_hbm.at[layer, base + b, :, part], c_buf.at[slot, :, part], sems.at[slot, j]
        )

    def each(b, act):
        n = count(b)
        for j in range(blocks):
            @pl.when(j < n)
            def _():
                act(copy(b, j))

    c_buf[...] = jnp.zeros_like(c_buf)
    for b in range(depth - 2):
        each(b, lambda c: c.start())

    def attend(b, t):
        slot = lax.rem(b, depth)
        q = q_ref[b]
        s = jnp.dot(q, c_buf[slot, :, 0:t], preferred_element_type=F32) * SCALE
        keep = lax.broadcasted_iota(jnp.int32, s.shape, 1) < length(b)
        s = jnp.where(keep, s, -jnp.inf)
        e = jnp.exp(s - jnp.max(s, axis=-1, keepdims=True))
        p = (e / jnp.sum(e, axis=-1, keepdims=True)).astype(BF16)
        o = lax.dot_general(
            c_buf[slot, 0:LAT, 0:t], p, (((1,), (1,)), ((), ())), preferred_element_type=F32
        )
        o_ref[b] = o.T.astype(BF16)

    @pl.loop(0, rows // 2)
    def _(i):
        b = 2 * i
        for k in range(2):
            @pl.when(b + depth - 2 + k < rows)
            def _():
                each(b + depth - 2 + k, lambda c: c.start())
        for k in range(2):
            each(b + k, lambda c: c.wait())
        n = jnp.maximum(count(b), count(b + 1))
        for m in range(1, blocks + 1):
            @pl.when(n == m)
            def _():
                attend(b, m * block)
                attend(b + 1, m * block)


def _layer_kernel(layer, last, o_ref, x_ref, an_ref, fn_ref, wo_hbm, w1_hbm, w3_hbm, w2_hbm, wq_hbm, *rest):
    outs, scratch = rest[: 1 if last else 2], rest[1 if last else 2:]
    (wo_buf, w1_buf, w3_buf, w2_buf, o_all, p_buf, pr1, pr2, g_all, a_buf, y_buf, yr1, yr2, yr3, x_buf, h_all,
     w_sems, ws_sems, o_sems, p_sems, g_sems, y_sems, h_sems, *more) = scratch
    here = Place()
    wo_copy = pltpu.make_async_copy(wo_hbm.at[layer], wo_buf, w_sems.at[0])
    wo_copy.start()
    own = [
        pltpu.make_async_copy(hbm.at[layer], buf.at[here.c], w_sems.at[1 + k])
        for k, (hbm, buf) in enumerate(((w3_hbm, w3_buf), (w1_hbm, w1_buf), (w2_hbm, w2_buf)))
    ]
    cube = [here.other(dx=dx, dz=dz, dy=dy) for dx, dz, dy in RING]
    partner = here.other(dc=1)
    _greet(cube + [partner])

    o_copies = []
    for k, (dz, dy) in enumerate(TP_PEERS):
        peer = here.other(dz=dz, dy=dy)
        o_copies.append(_send(o_ref.at[peer['tp']], o_all.at[here.tp], o_sems, k, peer))
    for copy in own:
        copy.start()
    swaps = [
        _send(hbm.at[layer], buf.at[here.c], ws_sems, k, partner)
        for k, (hbm, buf) in enumerate(((w3_hbm, w3_buf), (w1_hbm, w1_buf), (w2_hbm, w2_buf)))
    ]
    if not last:
        wq_buf, q_send, q_recv, wq_sems, q_sems = more
        wq_copies = _wq_start(layer + 1, wq_hbm, wq_buf, wq_sems)
    o_all[here.tp] = o_ref[here.tp]
    for copy in o_copies:
        copy.wait_recv()
    wo_copy.wait()

    heads, width = o_all.shape[1], p_buf.shape[-1]
    lhs = jnp.concatenate([o_all[:, h].reshape(-1, LAT) for h in range(heads)], axis=1)
    attn = Halving(here, ('z', 'y'), p_buf, (pr1, pr2), p_sems, TP_ORDERS)
    for n in range(len(TP_ORDERS)):
        part = slice(n * width, (n + 1) * width)
        p_buf[n] = jnp.dot(lhs, wo_buf[:, part], preferred_element_type=F32).reshape(p_buf.shape[1:])
        attn.send(n, 0)
    for n in range(len(TP_ORDERS)):
        attn.add(n, 0)
        attn.send(n, 1)
    x_mine = x_ref[here.tp] if layer == 0 else x_ref[...]
    for n in range(len(TP_ORDERS)):
        part = slice(n * width, (n + 1) * width)
        total = attn.add(n, 1).astype(BF16)
        x_buf[:, part] = (x_mine[:, part].astype(F32) + total.astype(F32)).astype(BF16)
    x_mid = x_buf[...]

    g_all[here.x, here.tp] = _norm(x_mid, fn_ref[layer:layer + 1, :])
    mine = g_all.at[here.x, here.tp]
    g_copies = [_send(mine, mine, g_sems, k, device) for k, device in enumerate(cube)]
    for copy in own:
        copy.wait()
    for copy in swaps:
        copy.wait_recv()
    for copy in g_copies:
        copy.wait_recv()

    g = g_all[...].reshape(-1, g_all.shape[-1])
    cols = w1_buf.shape[1]

    @pl.loop(0, 2)
    def _(s):
        for lo in range(0, cols, 256):
            part = slice(lo, min(lo + 256, cols))
            u = lax.dot_general(w3_buf[s, part, :], g, (((1,), (1,)), ((), ())), preferred_element_type=F32)
            v = lax.dot_general(w1_buf[s, part, :], g, (((1,), (1,)), ((), ())), preferred_element_type=F32)
            a_buf[s, :, part] = (u * jax.nn.sigmoid(u) * v).T.astype(BF16)

    ffn = Halving(here, ('x', 'z', 'y'), y_buf, (yr1, yr2, yr3), y_sems, CUBE_ORDERS)
    width = y_buf.shape[-1]
    for n in range(len(CUBE_ORDERS)):
        part = slice(n * width, (n + 1) * width)
        y = jnp.dot(a_buf[0], w2_buf[0, :, part], preferred_element_type=F32)
        y += jnp.dot(a_buf[1], w2_buf[1, :, part], preferred_element_type=F32)
        y_buf[n] = y.reshape(y_buf.shape[1:])
        ffn.send(n, 0)
    for phase in range(2):
        for n in range(len(CUBE_ORDERS)):
            ffn.add(n, phase)
            ffn.send(n, phase + 1)
    for n in range(len(CUBE_ORDERS)):
        part = slice(n * width, (n + 1) * width)
        total = ffn.add(n, 2).astype(BF16)
        x_buf[:, part] = (x_mid[:, part].astype(F32) + total.astype(F32)).astype(BF16)
    x_new = x_buf[...]

    h_all[here.tp] = x_new if last else _norm(x_new, an_ref[layer + 1:layer + 2, :])
    mine = h_all.at[here.tp]
    h_copies = [
        _send(mine, mine, h_sems, k, here.other(dz=dz, dy=dy)) for k, (dz, dy) in enumerate(TP_PEERS)
    ]
    for copy in h_copies:
        copy.wait_recv()
    if last:
        outs[0][...] = h_all[...]
    else:
        outs[1][...] = x_new
        h = h_all[...].reshape(-1, h_all.shape[-1])
        _q_exchange(here, h, wq_buf, wq_copies, q_send, q_recv, outs[0], q_sems)
    attn.finish()
    ffn.finish()
    for copy in o_copies + swaps + g_copies + h_copies:
        copy.wait_send()


VM = pl.BlockSpec(memory_space=pltpu.VMEM)
ANY = pl.BlockSpec(memory_space=pl.ANY)
DMA = pltpu.SemaphoreType.DMA


def solution(mesh):
    def body(x, lengths, cache, attn_norm, ffn_norm, wq, wo, w1, w3, w2):
        nb, d = x.shape
        n_layers, _, s_len, kv = cache.shape
        heads = wq.shape[2] // kv
        rows = nb // 4
        cols = w1.shape[2]
        q_shape = (4, rows, heads * kv)

        def params(cid):
            return pltpu.CompilerParams(collective_id=cid, has_side_effects=True, vmem_limit_bytes=VMEM_LIMIT)

        q_scratch = [
            pltpu.VMEM((d, heads * kv), BF16),
            pltpu.VMEM(q_shape, BF16),
            pltpu.VMEM(q_shape, BF16),
            DMA((3,)),
            DMA((2, 9)),
        ]

        q = pl.pallas_call(
            _first_kernel,
            out_shape=jax.ShapeDtypeStruct(q_shape, BF16),
            in_specs=[VM, VM, ANY],
            out_specs=VM,
            scratch_shapes=q_scratch,
            compiler_params=params(0),
            name='q_first',
        )(x, attn_norm, wq)

        cache_t = cache.transpose(0, 1, 3, 2)
        w1_t, w3_t = w1.transpose(0, 2, 1), w3.transpose(0, 2, 1)
        x_in = x.reshape(4, rows, d)
        for layer in range(n_layers):
            last = layer == n_layers - 1
            qt = q.reshape(4, rows, heads, kv).transpose(1, 0, 2, 3).reshape(rows, 4 * heads, kv)
            o = pl.pallas_call(
                functools.partial(_attention_kernel, layer),
                out_shape=jax.ShapeDtypeStruct((rows, 4 * heads, LAT), BF16),
                in_specs=[pl.BlockSpec(memory_space=pltpu.SMEM), VM, ANY],
                out_specs=VM,
                scratch_shapes=[pltpu.VMEM((8, kv, s_len), BF16), DMA((8, s_len // 128))],
                compiler_params=pltpu.CompilerParams(vmem_limit_bytes=VMEM_LIMIT),
                name='attention',
            )(lengths, qt, cache_t)
            ot = o.reshape(rows, 4, heads, LAT).transpose(1, 2, 0, 3)
            scratch = [
                pltpu.VMEM(wo.shape[1:], BF16),
                pltpu.VMEM((2, cols, d), BF16),
                pltpu.VMEM((2, cols, d), BF16),
                pltpu.VMEM((2, cols, d), BF16),
                pltpu.VMEM((4, heads, rows, LAT), BF16),
                pltpu.VMEM((4, 2, 2, rows, d // 4), F32),
                pltpu.VMEM((4, 2, rows, d // 4), F32),
                pltpu.VMEM((4, rows, d // 4), F32),
                pltpu.VMEM((2, 4, rows, d), BF16),
                pltpu.VMEM((2, 8 * rows, cols), BF16),
                pltpu.VMEM((8, 2, 2, 2, rows, d // 8), F32),
                pltpu.VMEM((8, 2, 2, rows, d // 8), F32),
                pltpu.VMEM((8, 2, rows, d // 8), F32),
                pltpu.VMEM((8, rows, d // 8), F32),
                pltpu.VMEM((rows, d), BF16),
                pltpu.VMEM((4, rows, d), BF16),
                DMA((4,)),
                DMA((2, 3)),
                DMA((2, 3)),
                DMA((2, 8)),
                DMA((2, 7)),
                DMA((2, 24)),
                DMA((2, 3)),
            ]
            if last:
                out_shape = [jax.ShapeDtypeStruct((4, rows, d), BF16)]
            else:
                out_shape = [jax.ShapeDtypeStruct(q_shape, BF16), jax.ShapeDtypeStruct((rows, d), BF16)]
                scratch += q_scratch
            outs = pl.pallas_call(
                functools.partial(_layer_kernel, layer, last),
                out_shape=out_shape,
                in_specs=[VM, VM, VM, VM, ANY, ANY, ANY, ANY, ANY],
                out_specs=[VM] * len(out_shape),
                scratch_shapes=scratch,
                compiler_params=params(1 + layer),
                name=f'layer_{layer}',
            )(ot, x_in, attn_norm, ffn_norm, wo, w1_t, w3_t, w2, wq)
            if last:
                return outs[0].reshape(nb, d)
            q, x_in = outs

    in_specs = (
        P('dp', None),
        P('dp'),
        P(None, 'dp', None, None),
        P(None, None),
        P(None, None),
        P(None, None, 'tp'),
        P(None, 'tp', None),
        P(None, None, ('dp', 'tp')),
        P(None, None, ('dp', 'tp')),
        P(None, ('dp', 'tp'), None),
    )
    return jax.shard_map(body, mesh=mesh, in_specs=in_specs, out_specs=P('dp', None), check_vma=False)
```

```python
import functools

import jax
import jax.numpy as jnp
from jax import lax
from jax.experimental import pallas as pl
from jax.experimental.pallas import tpu as pltpu
from jax.sharding import PartitionSpec as P

MESH = pl.DeviceIdType.MESH
F32 = jnp.float32
BF16 = jnp.bfloat16
LAT = 512
EPS = 1e-6
SCALE = 192 ** -0.5
VMEM_LIMIT = 64 * 1024 * 1024 - 65536

TP_ORDERS = (('z', 'y'), ('y', 'z'), ('z', 'y'), ('y', 'z'))
CUBE_ORDERS = (
    ('x', 'y', 'z'), ('y', 'z', 'x'), ('z', 'x', 'y'),
    ('x', 'y', 'z'), ('y', 'z', 'x'), ('z', 'x', 'y'),
    ('x', 'y', 'z'), ('y', 'z', 'x'),
)
RING = ((1, 0, 0), (0, 1, 0), (0, 0, 1), (0, 1, 1), (1, 1, 0), (1, 0, 1), (1, 1, 1))
TP_PEERS = ((1, 0), (0, 1), (1, 1))


class Place:
    def __init__(self):
        self.tp, self.dp = lax.axis_index('tp'), lax.axis_index('dp')
        self.z, self.y = lax.div(self.tp, 2), lax.rem(self.tp, 2)
        self.x, self.c = lax.div(self.dp, 2), lax.rem(self.dp, 2)
        self.at = {'x': self.x, 'z': self.z, 'y': self.y}

    def other(self, dx=0, dz=0, dy=0, dc=0):
        x = 1 - self.x if dx else self.x
        z = 1 - self.z if dz else self.z
        y = 1 - self.y if dy else self.y
        c = 1 - self.c if dc else self.c
        return {'tp': 2 * z + y, 'dp': 2 * x + c}

    def along(self, axis):
        return self.other(**{'d' + axis: 1})


def _send(src, dst, sems, k, device):
    copy = pltpu.make_async_remote_copy(
        src_ref=src, dst_ref=dst, send_sem=sems.at[0, k], recv_sem=sems.at[1, k],
        device_id=device, device_id_type=MESH,
    )
    copy.start()
    return copy


def _norm(v, w):
    vf = v.astype(F32)
    r = lax.rsqrt(jnp.mean(vf * vf, axis=-1, keepdims=True) + EPS)
    return (vf * r * w.astype(F32)).astype(BF16)


def _greet(devices):
    barrier = pltpu.get_barrier_semaphore()
    for device in devices:
        pl.semaphore_signal(barrier, inc=1, device_id=device, device_id_type=MESH)
    pl.semaphore_wait(barrier, len(devices))


class Halving:
    def __init__(self, here, axes, buf, recvs, sems, orders):
        self.here, self.axes, self.buf, self.recvs, self.sems, self.orders = here, axes, buf, recvs, sems, orders
        self.copies = {}

    def _view(self, chunk, phase, flip):
        index = [slice(None)] * len(self.axes)
        for p, axis in enumerate(self.orders[chunk][: phase + 1]):
            mine = self.here.at[axis]
            index[self.axes.index(axis)] = 1 - mine if (flip and p == phase) else mine
        return (chunk, *index)

    def send(self, chunk, phase):
        axis = self.orders[chunk][phase]
        self.copies[chunk, phase] = _send(
            self.buf.at[self._view(chunk, phase, True)], self.recvs[phase].at[chunk],
            self.sems, phase * len(self.orders) + chunk, self.here.along(axis),
        )

    def add(self, chunk, phase):
        self.copies[chunk, phase].wait_recv()
        view = self._view(chunk, phase, False)
        total = self.buf[view] + self.recvs[phase][chunk]
        if phase + 1 < len(self.axes):
            self.buf[view] = total
        return total

    def finish(self):
        for copy in self.copies.values():
            copy.wait_send()


def _kernel(
    len_ref, x_ref, an_ref, fn_ref, cache_hbm, wq_hbm, wo_hbm, w1_hbm, w3_hbm, w2_hbm, out_ref,
    wq_buf, wo_buf, w_buf, stage, c_buf, h_buf, q_send, q_recv, q_att, o_rows, o_send, o_all,
    p_buf, pr1, pr2, x_buf, g_all, g_buf, a_buf, y_buf, yr1, yr2, yr3, h_all,
    wq_sems, wo_sem, st_sems, ws_sems, c_sems, q_sems, o_sems, p_sems, g_sems, y_sems, h_sems, credit,
):
    here = Place()
    n_layers = cache_hbm.shape[0]
    d = x_buf.shape[1]
    rows = x_buf.shape[0]
    unit = c_buf.shape[1]
    units = rows // unit
    cols = w_buf.shape[2]
    chunk = stage.shape[1]
    heads = o_send.shape[2]
    kv = c_buf.shape[2]
    q_width = q_send.shape[-1] // 3
    partner = here.other(dc=1)
    peers = [here.other(dz=dz, dy=dy) for dz, dy in TP_PEERS]
    cube = [here.other(dx=dx, dz=dz, dy=dy) for dx, dz, dy in RING]

    def wq_copy(layer, n):
        part = slice(n * q_width, (n + 1) * q_width)
        return pltpu.make_async_copy(wq_hbm.at[layer, :, part], wq_buf.at[:, part], wq_sems.at[n])

    def wo_copy(layer):
        return pltpu.make_async_copy(wo_hbm.at[layer], wo_buf, wo_sem.at[0])

    def cache_copy(layer, i):
        slot = lax.rem(i, 2)
        return pltpu.make_async_copy(
            cache_hbm.at[layer, pl.ds(here.tp * rows + i * unit, unit)], c_buf.at[slot], c_sems.at[slot]
        )

    pieces = [
        (k, hbm, lo, min(chunk, cols - lo))
        for k, hbm in enumerate((w3_hbm, w1_hbm, w2_hbm)) for lo in range(0, cols, chunk)
    ]
    ring = stage.shape[0]

    def piece_copy(i):
        _, hbm, lo, n = pieces[i]
        return pltpu.make_async_copy(hbm.at[lo:lo + n], stage.at[i % ring, 0:n], st_sems.at[i % ring])

    def unpack(layer, i):
        k, _, lo, n = pieces[i]
        slot = i % ring

        @pl.loop(0, n // 16)
        def _(j):
            r = pl.multiple_of(j * 16, 16)
            pair = pltpu.einshape('alk->lak', stage[slot, pl.ds(r, 16)])
            w_buf[k, here.c, pl.ds(pl.multiple_of(lo + r, 16), 16), :] = pair[layer]
        if n % 16:
            r = n - n % 16
            pair = pltpu.einshape('alk->lak', stage[slot, r:n])
            w_buf[k, here.c, lo + r:lo + n, :] = pair[layer]

    for n in range(3):
        wq_copy(0, n).start()
    for i in range(2):
        cache_copy(0, i).start()
    for i in range(ring):
        piece_copy(i).start()
    wo_copy(0).start()
    _greet(cube + [partner])

    for layer in range(n_layers):
        last = layer + 1 == n_layers
        x_all = x_ref if layer == 0 else h_all

        for t in range(4):
            h_buf[t * rows:(t + 1) * rows, :] = _norm(x_all[t], an_ref[layer:layer + 1, :])
        q_copies = []
        for n in range(3):
            wq_copy(layer, n).wait()
            part = slice(n * q_width, (n + 1) * q_width)
            q = jnp.dot(h_buf[...], wq_buf[:, part], preferred_element_type=F32).astype(BF16)
            q_send[:, :, part] = q.reshape(4, rows, q_width)
            for k, peer in enumerate(peers):
                q_copies.append(_send(
                    q_send.at[peer['tp'], :, part], q_recv.at[here.tp, :, part], q_sems, 3 * n + k, peer,
                ))
        if not last:
            for n in range(3):
                wq_copy(layer + 1, n).start()
        q_recv[here.tp] = q_send[here.tp]

        swaps = []
        for i in range(len(pieces)):
            piece_copy(i).wait()
            unpack(layer, i)
            if i + ring < len(pieces):
                piece_copy(i + ring).start()
            k = pieces[i][0]
            if i + 1 == len(pieces) or pieces[i + 1][0] != k:
                if layer and k == 0:
                    pl.semaphore_wait(credit, 1)
                mine = w_buf.at[k, here.c]
                swaps.append(_send(mine, mine, ws_sems, k, partner))
        if not last:
            for i in range(ring):
                piece_copy(i).start()

        for copy in q_copies:
            copy.wait_recv()
        for h in range(heads):
            q = q_recv[:, :, h * kv:(h + 1) * kv]
            q_att[:, 4 * h:4 * h + 4, :] = pltpu.einshape('tbk->btk', q)

        def o_copy(i, k):
            return pltpu.make_async_remote_copy(
                src_ref=o_send.at[peers[k]['tp'], i], dst_ref=o_all.at[here.tp, i],
                send_sem=o_sems.at[0, 3 * i + k], recv_sem=o_sems.at[1, 3 * i + k],
                device_id=peers[k], device_id_type=MESH,
            )

        @pl.loop(0, units)
        def _(i):
            slot = lax.rem(i, 2)
            cache_copy(layer, i).wait()
            for lo in range(0, unit, 4):
                scores = [
                    jnp.dot(q_att[i * unit + k], c_buf[slot, k], preferred_element_type=F32)
                    for k in range(lo, lo + 4)
                ]
                probs = []
                for k, s in enumerate(scores, lo):
                    keep = lax.broadcasted_iota(jnp.int32, s.shape, 1) < len_ref[here.tp * rows + i * unit + k]
                    s = jnp.where(keep, s * SCALE, -jnp.inf)
                    e = jnp.exp(s - jnp.max(s, axis=-1, keepdims=True))
                    probs.append((e / jnp.sum(e, axis=-1, keepdims=True)).astype(BF16))
                for k, p in enumerate(probs, lo):
                    o = lax.dot_general(
                        p, c_buf[slot, k, 0:LAT, :], (((1,), (1,)), ((), ())), preferred_element_type=F32
                    )
                    for j in range(LAT // 128):
                        o_rows[j, k * 16:(k + 1) * 16, :] = o[:, j * 128:(j + 1) * 128]
            for h in range(heads):
                for t in range(4):
                    for j in range(LAT // 128):
                        part = slice(j * 128, (j + 1) * 128)
                        o_send[t, i, h, :, part] = o_rows[j, pl.ds(4 * h + t, unit, stride=16), :].astype(BF16)
            for k in range(3):
                o_copy(i, k).start()
            o_all[here.tp, i] = o_send[here.tp, i]

            @pl.when(i + 2 < units)
            def _():
                cache_copy(layer, i + 2).start()
        if not last:
            for i in range(2):
                cache_copy(layer + 1, i).start()
        wo_copy(layer).wait()
        for i in range(units):
            for k in range(3):
                o_copy(i, k).wait_recv()

        width = p_buf.shape[-1]
        lhs = jnp.concatenate([o_all[:, :, h].reshape(4 * rows, LAT) for h in range(heads)], axis=1)
        attn = Halving(here, ('z', 'y'), p_buf, (pr1, pr2), p_sems, TP_ORDERS)
        for n in range(len(TP_ORDERS)):
            part = slice(n * width, (n + 1) * width)
            p_buf[n] = jnp.dot(lhs, wo_buf[:, part], preferred_element_type=F32).reshape(p_buf.shape[1:])
            attn.send(n, 0)
        if not last:
            wo_copy(layer + 1).start()
        for n in range(len(TP_ORDERS)):
            attn.add(n, 0)
            attn.send(n, 1)
        x_mine = x_ref[here.tp] if layer == 0 else x_buf[...]
        g_copies = []
        for n in range(len(TP_ORDERS)):
            part = slice(n * width, (n + 1) * width)
            total = attn.add(n, 1).astype(BF16)
            x_part = (x_mine[:, part].astype(F32) + total.astype(F32)).astype(BF16)
            x_buf[:, part] = x_part
            g_all[here.x, here.tp, :, part] = x_part
            mine = g_all.at[here.x, here.tp, :, part]
            g_copies.append([_send(mine, mine, g_sems, 7 * n + k, device) for k, device in enumerate(cube)])

        def g_norm(x, t):
            at = pl.multiple_of((4 * x + t) * rows, rows)
            g_buf[pl.ds(at, rows), :] = _norm(g_all[x, t], fn_ref[layer:layer + 1, :])

        g_norm(here.x, here.tp)
        for copy in swaps:
            copy.wait_recv()
        for k, device in enumerate(cube):
            for copies in g_copies:
                copies[k].wait_recv()
            g_norm(lax.div(device['dp'], 2), device['tp'])

        @pl.loop(0, 2)
        def _(s):
            for lo in range(0, cols, 256):
                part = slice(lo, min(lo + 256, cols))
                u, v = (
                    lax.dot_general(
                        w_buf[k, s, part, :], g_buf[...], (((1,), (1,)), ((), ())), preferred_element_type=F32
                    ) for k in range(2)
                )
                a_buf[s, :, part] = (u * jax.nn.sigmoid(u) * v).T.astype(BF16)

        ffn = Halving(here, ('x', 'z', 'y'), y_buf, (yr1, yr2, yr3), y_sems, CUBE_ORDERS)
        width = y_buf.shape[-1]
        for n in range(len(CUBE_ORDERS)):
            part = slice(n * width, (n + 1) * width)
            y = jnp.dot(a_buf[0], w_buf[2, 0, :, part], preferred_element_type=F32)
            y += jnp.dot(a_buf[1], w_buf[2, 1, :, part], preferred_element_type=F32)
            y_buf[n] = y.reshape(y_buf.shape[1:])
            ffn.send(n, 0)
        if not last:
            pl.semaphore_signal(credit, inc=1, device_id=partner, device_id_type=MESH)
        for phase in range(2):
            for n in range(len(CUBE_ORDERS)):
                ffn.add(n, phase)
                ffn.send(n, phase + 1)
        h_copies = []
        for n in range(len(CUBE_ORDERS)):
            part = slice(n * width, (n + 1) * width)
            total = ffn.add(n, 2).astype(BF16)
            x_part = (x_buf[:, part].astype(F32) + total.astype(F32)).astype(BF16)
            x_buf[:, part] = x_part
            h_all[here.tp, :, part] = x_part
            mine = h_all.at[here.tp, :, part]
            h_copies += [_send(mine, mine, h_sems, 3 * n + k, peer) for k, peer in enumerate(peers)]

        for copy in h_copies:
            copy.wait_recv()
        attn.finish()
        ffn.finish()
        for copy in q_copies + swaps + h_copies + [copy for copies in g_copies for copy in copies]:
            copy.wait_send()
        for i in range(units):
            for k in range(3):
                o_copy(i, k).wait_send()
    out_ref[...] = h_all[...]


VM = pl.BlockSpec(memory_space=pltpu.VMEM)
SM = pl.BlockSpec(memory_space=pltpu.SMEM)
ANY = pl.BlockSpec(memory_space=pl.ANY)
DMA = pltpu.SemaphoreType.DMA


def solution(mesh):
    def body(x, lengths, cache, attn_norm, ffn_norm, wq, wo, w1, w3, w2):
        nb, d = x.shape
        s_len, kv = cache.shape[2:]
        heads = wq.shape[2] // kv
        rows = nb // 4
        cols = w1.shape[2]
        unit = 8
        q_shape = (4, rows, heads * kv)
        scratch = [
            pltpu.VMEM(wq.shape[1:], BF16),
            pltpu.VMEM(wo.shape[1:], BF16),
            pltpu.VMEM((3, 2, cols, d), BF16),
            pltpu.VMEM((2, 176, 2, d), BF16),
            pltpu.VMEM((2, unit, kv, s_len), BF16),
            pltpu.VMEM((nb, d), BF16),
            pltpu.VMEM(q_shape, BF16),
            pltpu.VMEM(q_shape, BF16),
            pltpu.VMEM((rows, 4 * heads, kv), BF16),
            pltpu.VMEM((LAT // 128, unit * 4 * heads, 128), F32),
            pltpu.VMEM((4, rows // unit, heads, unit, LAT), BF16),
            pltpu.VMEM((4, rows // unit, heads, unit, LAT), BF16),
            pltpu.VMEM((4, 2, 2, rows, d // 4), F32),
            pltpu.VMEM((4, 2, rows, d // 4), F32),
            pltpu.VMEM((4, rows, d // 4), F32),
            pltpu.VMEM((rows, d), BF16),
            pltpu.VMEM((2, 4, rows, d), BF16),
            pltpu.VMEM((8 * rows, d), BF16),
            pltpu.VMEM((2, 8 * rows, cols), BF16),
            pltpu.VMEM((8, 2, 2, 2, rows, d // 8), F32),
            pltpu.VMEM((8, 2, 2, rows, d // 8), F32),
            pltpu.VMEM((8, 2, rows, d // 8), F32),
            pltpu.VMEM((8, rows, d // 8), F32),
            pltpu.VMEM((4, rows, d), BF16),
            DMA((3,)),
            DMA((1,)),
            DMA((2,)),
            DMA((2, 3)),
            DMA((2,)),
            DMA((2, 9)),
            DMA((2, 12)),
            DMA((2, 8)),
            DMA((2, 28)),
            DMA((2, 24)),
            DMA((2, 24)),
            pltpu.SemaphoreType.REGULAR,
        ]
        out = pl.pallas_call(
            _kernel,
            out_shape=jax.ShapeDtypeStruct((4, rows, d), BF16),
            in_specs=[SM, VM, VM, VM] + [ANY] * 6,
            out_specs=VM,
            scratch_shapes=scratch,
            compiler_params=pltpu.CompilerParams(
                collective_id=0, has_side_effects=True, vmem_limit_bytes=VMEM_LIMIT,
            ),
            name='two_layers',
        )(
            lengths, x.reshape(4, rows, d), attn_norm, ffn_norm, cache.transpose(0, 1, 3, 2), wq, wo,
            w1.transpose(2, 0, 1), w3.transpose(2, 0, 1), w2.transpose(1, 0, 2),
        )
        return out.reshape(nb, d)

    in_specs = (
        P('dp', None),
        P('dp'),
        P(None, 'dp', None, None),
        P(None, None),
        P(None, None),
        P(None, None, 'tp'),
        P(None, 'tp', None),
        P(None, None, ('dp', 'tp')),
        P(None, None, ('dp', 'tp')),
        P(None, ('dp', 'tp'), None),
    )
    return jax.shard_map(body, mesh=mesh, in_specs=in_specs, out_specs=P('dp', None), check_vma=False)
```

```python
import functools

import jax
import jax.numpy as jnp
from jax import lax
from jax.experimental import pallas as pl
from jax.experimental.pallas import tpu as pltpu
from jax.sharding import PartitionSpec as P

MESH = pl.DeviceIdType.MESH
F32 = jnp.float32
BF16 = jnp.bfloat16
LAT = 512
EPS = 1e-6
SCALE = 192 ** -0.5
VMEM_LIMIT = 64 * 1024 * 1024 - 65536

TP_ORDERS = (('z', 'y'), ('y', 'z')) * 4
GATHER_ORDERS = (
    ('y', 'z', 'x'), ('z', 'y', 'x'), ('y', 'z', 'x'), ('z', 'y', 'x'),
    ('y', 'z', 'x'), ('z', 'x', 'y'), ('x', 'y', 'z'), ('x', 'z', 'y'),
)
CUBE_ORDERS = (
    ('x', 'y', 'z'), ('y', 'z', 'x'), ('z', 'x', 'y'),
    ('x', 'y', 'z'), ('y', 'z', 'x'), ('z', 'x', 'y'),
    ('x', 'y', 'z'), ('y', 'z', 'x'),
)
NEAR = ((1, 0, 0), (0, 1, 0), (0, 0, 1), (0, 1, 1), (1, 1, 0), (1, 0, 1), (1, 1, 1))
TP_PEERS = ((1, 0), (0, 1), (1, 1))


class Place:
    def __init__(self):
        self.tp, self.dp = lax.axis_index('tp'), lax.axis_index('dp')
        self.z, self.y = lax.div(self.tp, 2), lax.rem(self.tp, 2)
        self.x, self.c = lax.div(self.dp, 2), lax.rem(self.dp, 2)
        self.at = {'x': self.x, 'z': self.z, 'y': self.y}

    def other(self, dx=0, dz=0, dy=0, dc=0):
        x = 1 - self.x if dx else self.x
        z = 1 - self.z if dz else self.z
        y = 1 - self.y if dy else self.y
        c = 1 - self.c if dc else self.c
        return {'tp': 2 * z + y, 'dp': 2 * x + c}

    def along(self, axis):
        return self.other(**{'d' + axis: 1})


def _send(src, dst, sems, k, device):
    copy = pltpu.make_async_remote_copy(
        src_ref=src, dst_ref=dst, send_sem=sems.at[0, k], recv_sem=sems.at[1, k],
        device_id=device, device_id_type=MESH,
    )
    copy.start()
    return copy


def _norm(v, w):
    vf = v.astype(F32)
    r = lax.rsqrt(jnp.mean(vf * vf, axis=-1, keepdims=True) + EPS)
    return (vf * r * w.astype(F32)).astype(BF16)


def _greet(devices):
    barrier = pltpu.get_barrier_semaphore()
    for device in devices:
        pl.semaphore_signal(barrier, inc=1, device_id=device, device_id_type=MESH)
    pl.semaphore_wait(barrier, len(devices))


class Halving:
    def __init__(self, here, axes, buf, recvs, sems, orders):
        self.here, self.axes, self.buf, self.recvs, self.sems, self.orders = here, axes, buf, recvs, sems, orders
        self.copies = {}

    def _view(self, chunk, phase, flip):
        index = [slice(None)] * len(self.axes)
        for p, axis in enumerate(self.orders[chunk][: phase + 1]):
            mine = self.here.at[axis]
            index[self.axes.index(axis)] = 1 - mine if (flip and p == phase) else mine
        return (chunk, *index)

    def send(self, chunk, phase):
        axis = self.orders[chunk][phase]
        self.copies[chunk, phase] = _send(
            self.buf.at[self._view(chunk, phase, True)], self.recvs[phase].at[chunk],
            self.sems, phase * len(self.orders) + chunk, self.here.along(axis),
        )

    def add(self, chunk, phase):
        self.copies[chunk, phase].wait_recv()
        view = self._view(chunk, phase, False)
        total = self.buf[view] + self.recvs[phase][chunk]
        if phase + 1 < len(self.axes):
            self.buf[view] = total
        return total

    def finish(self):
        for copy in self.copies.values():
            copy.wait_send()


class Doubling:
    def __init__(self, here, axes, buf, sems, orders):
        self.here, self.axes, self.buf, self.sems, self.orders = here, axes, buf, sems, orders
        self.copies = {}

    def send(self, chunk, phase):
        order = self.orders[chunk]
        held = order[:phase]
        part = self.buf.at[(chunk, *(slice(None) if axis in held else self.here.at[axis] for axis in self.axes))]
        self.copies[chunk, phase] = _send(
            part, part, self.sems, phase * len(self.orders) + chunk, self.here.along(order[phase]),
        )

    def wait(self, chunk, phase):
        self.copies[chunk, phase].wait_recv()

    def finish(self):
        for copy in self.copies.values():
            copy.wait_send()


def _skewed(count, stages, lag, filler=()):
    filler = list(filler)
    for step in range(count + lag * (len(stages) - 1)):
        for k in reversed(range(len(stages))):
            if 0 <= step - k * lag < count:
                stages[k](step - k * lag)
        if filler:
            filler.pop(0)()
    for work in filler:
        work()


def _kernel(
    len_ref, x_ref, an_ref, fn_ref, cache_hbm, wq_hbm, wo_hbm, w1_hbm, w3_hbm, w2_hbm, out_ref,
    wq_buf, wo_buf, w_buf, stage, c_buf, h_buf, q_send, q_recv, q_att, o_rows, o_send, o_all,
    p_buf, pr1, pr2, x_buf, g_all, g_buf, a_buf, y_buf, yr1, yr2, yr3, h_all,
    wq_sems, wo_sem, st_sems, ws_sems, c_sems, q_sems, o_sems, p_sems, g_sems, y_sems, h_sems, credit,
):
    here = Place()
    n_layers = cache_hbm.shape[0]
    d = x_buf.shape[1]
    rows = x_buf.shape[0]
    unit = c_buf.shape[1]
    units = rows // unit
    cols = w_buf.shape[2]
    chunk = stage.shape[1]
    heads = o_send.shape[2]
    kv = c_buf.shape[2]
    q_width = q_send.shape[-1] // 3
    chunks = len(CUBE_ORDERS)
    width = d // chunks
    swaps = []
    partner = here.other(dc=1)
    peers = [here.other(dz=dz, dy=dy) for dz, dy in TP_PEERS]
    cube = [here.other(dx=dx, dz=dz, dy=dy) for dx, dz, dy in NEAR]

    def wq_copy(layer, n):
        part = slice(n * q_width, (n + 1) * q_width)
        return pltpu.make_async_copy(wq_hbm.at[layer, :, part], wq_buf.at[:, part], wq_sems.at[n])

    def wo_copy(layer):
        return pltpu.make_async_copy(wo_hbm.at[layer], wo_buf, wo_sem.at[0])

    def cache_copy(layer, i):
        slot = lax.rem(i, 2)
        return pltpu.make_async_copy(
            cache_hbm.at[layer, pl.ds(here.tp * rows + i * unit, unit)], c_buf.at[slot], c_sems.at[slot]
        )

    pieces = [
        (k, hbm, lo, min(chunk, cols - lo))
        for k, hbm in enumerate((w3_hbm, w1_hbm, w2_hbm)) for lo in range(0, cols, chunk)
    ]
    ring = stage.shape[0]

    def piece_copy(i):
        _, hbm, lo, n = pieces[i]
        return pltpu.make_async_copy(hbm.at[lo:lo + n], stage.at[i % ring, 0:n], st_sems.at[i % ring])

    def unpack(layer, i):
        k, _, lo, n = pieces[i]
        slot = i % ring

        @pl.loop(0, n // 16)
        def _(j):
            r = pl.multiple_of(j * 16, 16)
            pair = pltpu.einshape('alk->lak', stage[slot, pl.ds(r, 16)])
            w_buf[k, here.c, pl.ds(pl.multiple_of(lo + r, 16), 16), :] = pair[layer]
        if n % 16:
            r = n - n % 16
            pair = pltpu.einshape('alk->lak', stage[slot, r:n])
            w_buf[k, here.c, lo + r:lo + n, :] = pair[layer]

    def share(layer, i):
        piece_copy(i).wait()
        unpack(layer, i)
        if i + ring < len(pieces):
            piece_copy(i + ring).start()
        elif layer + 1 < n_layers:
            piece_copy(i + ring - len(pieces)).start()
        k = pieces[i][0]
        if i + 1 == len(pieces) or pieces[i + 1][0] != k:
            if layer and k == 0:
                pl.semaphore_wait(credit, 1)
            mine = w_buf.at[k, here.c]
            swaps.append(_send(mine, mine, ws_sems, k, partner))

    def exchange(src, dst, sems, i, k):
        return pltpu.make_async_remote_copy(
            src_ref=src.at[peers[k]['tp'], i], dst_ref=dst.at[here.tp, i],
            send_sem=sems.at[0, 3 * i + k], recv_sem=sems.at[1, 3 * i + k],
            device_id=peers[k], device_id_type=MESH,
        )

    q_copy = functools.partial(exchange, q_send, q_recv, q_sems)
    o_copy = functools.partial(exchange, o_send, o_all, o_sems)

    for n in range(3):
        wq_copy(0, n).start()
    for i in range(2):
        cache_copy(0, i).start()
    for i in range(ring):
        piece_copy(i).start()
    wo_copy(0).start()
    _greet(cube + [partner])

    for layer in range(n_layers):
        last = layer + 1 == n_layers
        x_all = x_ref if layer == 0 else h_all

        for t in range(4):
            h_buf[t * rows:(t + 1) * rows, :] = _norm(x_all[t], an_ref[layer:layer + 1, :])
        for n in range(3):
            wq_copy(layer, n).wait()
            part = slice(n * q_width, (n + 1) * q_width)
            q = jnp.dot(h_buf[...], wq_buf[:, part], preferred_element_type=F32).astype(BF16)
            q_send[:, :, :, part] = q.reshape(4, units, unit, q_width)
        for i in range(units):
            for k in range(3):
                q_copy(i, k).start()
        if not last:
            for n in range(3):
                wq_copy(layer + 1, n).start()
        q_recv[here.tp] = q_send[here.tp]

        if layer == 0:
            for i in range(len(pieces)):
                share(0, i)

        @pl.loop(0, units)
        def _(i):
            slot = lax.rem(i, 2)
            for k in range(3):
                q_copy(i, k).wait_recv()
            for h in range(heads):
                q = q_recv[:, i, :, h * kv:(h + 1) * kv]
                q_att[:, 4 * h:4 * h + 4, :] = pltpu.einshape('tbk->btk', q)
            cache_copy(layer, i).wait()
            for lo in range(0, unit, 4):
                scores = [
                    jnp.dot(q_att[k], c_buf[slot, k], preferred_element_type=F32)
                    for k in range(lo, lo + 4)
                ]
                probs = []
                for k, s in enumerate(scores, lo):
                    keep = lax.broadcasted_iota(jnp.int32, s.shape, 1) < len_ref[here.tp * rows + i * unit + k]
                    s = jnp.where(keep, s * SCALE, -jnp.inf)
                    e = jnp.exp(s - jnp.max(s, axis=-1, keepdims=True))
                    probs.append((e / jnp.sum(e, axis=-1, keepdims=True)).astype(BF16))
                for k, p in enumerate(probs, lo):
                    o = lax.dot_general(
                        p, c_buf[slot, k, 0:LAT, :], (((1,), (1,)), ((), ())), preferred_element_type=F32
                    )
                    for j in range(LAT // 128):
                        o_rows[j, k * 16:(k + 1) * 16, :] = o[:, j * 128:(j + 1) * 128]
            for h in range(heads):
                for t in range(4):
                    for j in range(LAT // 128):
                        part = slice(j * 128, (j + 1) * 128)
                        o_send[t, i, h, :, part] = o_rows[j, pl.ds(4 * h + t, unit, stride=16), :].astype(BF16)
            for k in range(3):
                o_copy(i, k).start()
            o_all[here.tp, i] = o_send[here.tp, i]

            @pl.when(i + 2 < units)
            def _():
                cache_copy(layer, i + 2).start()
        if not last:
            for i in range(2):
                cache_copy(layer + 1, i).start()
        wo_copy(layer).wait()
        for i in range(units):
            for k in range(3):
                o_copy(i, k).wait_recv()

        lhs = jnp.concatenate([o_all[:, :, h].reshape(4 * rows, LAT) for h in range(heads)], axis=1)
        attn = Halving(here, ('z', 'y'), p_buf, (pr1, pr2), p_sems, TP_ORDERS)
        gather = Doubling(here, ('x', 'z', 'y'), g_all, g_sems, GATHER_ORDERS)
        for n in range(0, chunks, 2):
            part = slice(n * width, (n + 2) * width)
            y = jnp.dot(lhs, wo_buf[:, part], preferred_element_type=F32)
            for k in range(2):
                p_buf[n + k] = y[:, k * width:(k + 1) * width].reshape(p_buf.shape[1:])
                attn.send(n + k, 0)
        if not last:
            wo_copy(layer + 1).start()
        x_mine = x_ref[here.tp] if layer == 0 else x_buf[...]

        def attn_first(n):
            attn.add(n, 0)
            attn.send(n, 1)

        def attn_last(n):
            part = slice(n * width, (n + 1) * width)
            total = attn.add(n, 1).astype(BF16)
            x_part = (x_mine[:, part].astype(F32) + total.astype(F32)).astype(BF16)
            x_buf[:, part] = x_part
            g_all[n, here.x, here.z, here.y] = x_part
            gather.send(n, 0)

        def pass_on(phase, n):
            gather.wait(n, phase)
            if phase < 2:
                gather.send(n, phase + 1)

        _skewed(chunks, [attn_first, attn_last] + [functools.partial(pass_on, phase) for phase in range(3)], 2)

        for x in range(2):
            for t in range(4):
                block = jnp.concatenate([g_all[n, x, t // 2, t % 2] for n in range(chunks)], axis=1)
                at = (4 * x + t) * rows
                g_buf[at:at + rows, :] = _norm(block, fn_ref[layer:layer + 1, :])
        for copy in swaps:
            copy.wait()
        swaps.clear()

        @pl.loop(0, 2)
        def _(s):
            for lo in range(0, cols, 256):
                part = slice(lo, min(lo + 256, cols))
                u, v = (
                    lax.dot_general(
                        w_buf[k, s, part, :], g_buf[...], (((1,), (1,)), ((), ())), preferred_element_type=F32
                    ) for k in range(2)
                )
                a_buf[s, :, part] = (u * jax.nn.sigmoid(u) * v).T.astype(BF16)

        ffn = Halving(here, ('x', 'z', 'y'), y_buf, (yr1, yr2, yr3), y_sems, CUBE_ORDERS)
        for n in range(chunks):
            part = slice(n * width, (n + 1) * width)
            y = jnp.dot(a_buf[0], w_buf[2, 0, :, part], preferred_element_type=F32)
            y += jnp.dot(a_buf[1], w_buf[2, 1, :, part], preferred_element_type=F32)
            y_buf[n] = y.reshape(y_buf.shape[1:])
            ffn.send(n, 0)
        if not last:
            pl.semaphore_signal(credit, inc=1, device_id=partner, device_id_type=MESH)
        h_copies = []

        def ffn_next(phase, n):
            ffn.add(n, phase)
            ffn.send(n, phase + 1)

        def ffn_last(n):
            part = slice(n * width, (n + 1) * width)
            total = ffn.add(n, 2).astype(BF16)
            x_part = (x_buf[:, part].astype(F32) + total.astype(F32)).astype(BF16)
            x_buf[:, part] = x_part
            h_all[here.tp, :, part] = x_part
            mine = h_all.at[here.tp, :, part]
            h_copies.extend(_send(mine, mine, h_sems, 3 * n + k, peer) for k, peer in enumerate(peers))

        filler = [] if last else [functools.partial(share, layer + 1, i) for i in range(len(pieces))]
        _skewed(chunks, [functools.partial(ffn_next, 0), functools.partial(ffn_next, 1), ffn_last], 2, filler)

        for copy in h_copies:
            copy.wait_recv()
        attn.finish()
        gather.finish()
        ffn.finish()
        for copy in h_copies:
            copy.wait_send()
        for i in range(units):
            for k in range(3):
                q_copy(i, k).wait_send()
                o_copy(i, k).wait_send()
    out_ref[...] = h_all[...]


VM = pl.BlockSpec(memory_space=pltpu.VMEM)
SM = pl.BlockSpec(memory_space=pltpu.SMEM)
ANY = pl.BlockSpec(memory_space=pl.ANY)
DMA = pltpu.SemaphoreType.DMA


def solution(mesh):
    def body(x, lengths, cache, attn_norm, ffn_norm, wq, wo, w1, w3, w2):
        nb, d = x.shape
        s_len, kv = cache.shape[2:]
        heads = wq.shape[2] // kv
        rows = nb // 4
        cols = w1.shape[2]
        unit = 8
        q_shape = (4, rows // unit, unit, heads * kv)
        scratch = [
            pltpu.VMEM(wq.shape[1:], BF16),
            pltpu.VMEM(wo.shape[1:], BF16),
            pltpu.VMEM((3, 2, cols, d), BF16),
            pltpu.VMEM((2, 176, 2, d), BF16),
            pltpu.VMEM((2, unit, kv, s_len), BF16),
            pltpu.VMEM((nb, d), BF16),
            pltpu.VMEM(q_shape, BF16),
            pltpu.VMEM(q_shape, BF16),
            pltpu.VMEM((unit, 4 * heads, kv), BF16),
            pltpu.VMEM((LAT // 128, unit * 4 * heads, 128), F32),
            pltpu.VMEM((4, rows // unit, heads, unit, LAT), BF16),
            pltpu.VMEM((4, rows // unit, heads, unit, LAT), BF16),
            pltpu.VMEM((8, 2, 2, rows, d // 8), F32),
            pltpu.VMEM((8, 2, rows, d // 8), F32),
            pltpu.VMEM((8, rows, d // 8), F32),
            pltpu.VMEM((rows, d), BF16),
            pltpu.VMEM((8, 2, 2, 2, rows, d // 8), BF16),
            pltpu.VMEM((8 * rows, d), BF16),
            pltpu.VMEM((2, 8 * rows, cols), BF16),
            pltpu.VMEM((8, 2, 2, 2, rows, d // 8), F32),
            pltpu.VMEM((8, 2, 2, rows, d // 8), F32),
            pltpu.VMEM((8, 2, rows, d // 8), F32),
            pltpu.VMEM((8, rows, d // 8), F32),
            pltpu.VMEM((4, rows, d), BF16),
            DMA((3,)),
            DMA((1,)),
            DMA((2,)),
            DMA((2, 3)),
            DMA((2,)),
            DMA((2, 12)),
            DMA((2, 12)),
            DMA((2, 16)),
            DMA((2, 24)),
            DMA((2, 24)),
            DMA((2, 24)),
            pltpu.SemaphoreType.REGULAR,
        ]
        out = pl.pallas_call(
            _kernel,
            out_shape=jax.ShapeDtypeStruct((4, rows, d), BF16),
            in_specs=[SM, VM, VM, VM] + [ANY] * 6,
            out_specs=VM,
            scratch_shapes=scratch,
            compiler_params=pltpu.CompilerParams(
                collective_id=0, has_side_effects=True, vmem_limit_bytes=VMEM_LIMIT,
            ),
            name='two_layers',
        )(
            lengths, x.reshape(4, rows, d), attn_norm, ffn_norm, cache.transpose(0, 1, 3, 2), wq, wo,
            w1.transpose(2, 0, 1), w3.transpose(2, 0, 1), w2.transpose(1, 0, 2),
        )
        return out.reshape(nb, d)

    in_specs = (
        P('dp', None),
        P('dp'),
        P(None, 'dp', None, None),
        P(None, None),
        P(None, None),
        P(None, None, 'tp'),
        P(None, 'tp', None),
        P(None, None, ('dp', 'tp')),
        P(None, None, ('dp', 'tp')),
        P(None, ('dp', 'tp'), None),
    )
    return jax.shard_map(body, mesh=mesh, in_specs=in_specs, out_specs=P('dp', None), check_vma=False)
```

```python
import functools

import jax
import jax.numpy as jnp
from jax import lax
from jax.experimental import pallas as pl
from jax.experimental.pallas import tpu as pltpu
from jax.sharding import PartitionSpec as P

MESH = pl.DeviceIdType.MESH
F32 = jnp.float32
BF16 = jnp.bfloat16
LAT = 512
EPS = 1e-6
SCALE = 192 ** -0.5
VMEM_LIMIT = 64 * 1024 * 1024 - 65536

TP_ORDERS = (('z', 'y'), ('y', 'z')) * 2
CUBE_ORDERS = (
    ('x', 'y', 'z'), ('y', 'z', 'x'), ('z', 'x', 'y'),
    ('x', 'y', 'z'), ('y', 'z', 'x'), ('z', 'x', 'y'),
    ('x', 'y', 'z'), ('y', 'z', 'x'),
)
NEAR = ((1, 0, 0), (0, 1, 0), (0, 0, 1), (0, 1, 1), (1, 1, 0), (1, 0, 1), (1, 1, 1))
TP_PEERS = ((1, 0), (0, 1), (1, 1))


class Place:
    def __init__(self):
        self.tp, self.dp = lax.axis_index('tp'), lax.axis_index('dp')
        self.z, self.y = lax.div(self.tp, 2), lax.rem(self.tp, 2)
        self.x, self.c = lax.div(self.dp, 2), lax.rem(self.dp, 2)
        self.at = {'x': self.x, 'z': self.z, 'y': self.y}

    def other(self, dx=0, dz=0, dy=0, dc=0):
        x = 1 - self.x if dx else self.x
        z = 1 - self.z if dz else self.z
        y = 1 - self.y if dy else self.y
        c = 1 - self.c if dc else self.c
        return {'tp': 2 * z + y, 'dp': 2 * x + c}

    def along(self, axis):
        return self.other(**{'d' + axis: 1})


def _send(src, dst, sems, k, device):
    copy = pltpu.make_async_remote_copy(
        src_ref=src, dst_ref=dst, send_sem=sems.at[0, k], recv_sem=sems.at[1, k],
        device_id=device, device_id_type=MESH,
    )
    copy.start()
    return copy


def _norm(v, w):
    vf = v.astype(F32)
    r = lax.rsqrt(jnp.mean(vf * vf, axis=-1, keepdims=True) + EPS)
    return (vf * r * w.astype(F32)).astype(BF16)


def _greet(devices):
    barrier = pltpu.get_barrier_semaphore()
    for device in devices:
        pl.semaphore_signal(barrier, inc=1, device_id=device, device_id_type=MESH)
    pl.semaphore_wait(barrier, len(devices))


class Halving:
    def __init__(self, here, axes, buf, recvs, sems, orders):
        self.here, self.axes, self.buf, self.recvs, self.sems, self.orders = here, axes, buf, recvs, sems, orders
        self.copies = {}

    def _view(self, chunk, phase, flip):
        index = [slice(None)] * len(self.axes)
        for p, axis in enumerate(self.orders[chunk][: phase + 1]):
            mine = self.here.at[axis]
            index[self.axes.index(axis)] = 1 - mine if (flip and p == phase) else mine
        return (chunk, *index)

    def send(self, chunk, phase):
        axis = self.orders[chunk][phase]
        self.copies[chunk, phase] = _send(
            self.buf.at[self._view(chunk, phase, True)], self.recvs[phase].at[chunk],
            self.sems, phase * len(self.orders) + chunk, self.here.along(axis),
        )

    def add(self, chunk, phase):
        self.copies[chunk, phase].wait_recv()
        view = self._view(chunk, phase, False)
        total = self.buf[view] + self.recvs[phase][chunk]
        if phase + 1 < len(self.axes):
            self.buf[view] = total
        return total

    def finish(self):
        for copy in self.copies.values():
            copy.wait_send()


def _kernel(
    len_ref, x_ref, an_ref, fn_ref, cache_hbm, wq_hbm, wo_hbm, w1_hbm, w3_hbm, w2_hbm, out_ref,
    wq_buf, wo_buf, w_buf, stage, c_buf, h_buf, q_send, q_recv, q_att, o_rows, o_send, o_all,
    p_buf, pr1, pr2, x_buf, g_all, g_buf, a_buf, y_buf, yr1, yr2, yr3, h_all,
    wq_sems, wo_sem, st_sems, ws_sems, c_sems, q_sems, o_sems, p_sems, g_sems, y_sems, h_sems, credit,
):
    here = Place()
    n_layers = cache_hbm.shape[0]
    d = x_buf.shape[1]
    rows = x_buf.shape[0]
    unit = c_buf.shape[1]
    units = rows // unit
    cols = w_buf.shape[2]
    chunk = stage.shape[1]
    heads = o_send.shape[2]
    kv = c_buf.shape[2]
    q_width = q_send.shape[-1] // 3
    chunks = len(CUBE_ORDERS)
    width = d // chunks
    swaps = []
    partner = here.other(dc=1)
    peers = [here.other(dz=dz, dy=dy) for dz, dy in TP_PEERS]
    cube = [here.other(dx=dx, dz=dz, dy=dy) for dx, dz, dy in NEAR]

    def wq_copy(layer, n):
        part = slice(n * q_width, (n + 1) * q_width)
        return pltpu.make_async_copy(wq_hbm.at[layer, :, part], wq_buf.at[:, part], wq_sems.at[n])

    def wo_copy(layer):
        return pltpu.make_async_copy(wo_hbm.at[layer], wo_buf, wo_sem.at[0])

    def cache_copy(layer, i):
        slot = lax.rem(i, 2)
        return pltpu.make_async_copy(
            cache_hbm.at[layer, pl.ds(here.tp * rows + i * unit, unit)], c_buf.at[slot], c_sems.at[slot]
        )

    pieces = [
        (k, hbm, lo, min(chunk, cols - lo))
        for k, hbm in enumerate((w3_hbm, w1_hbm, w2_hbm)) for lo in range(0, cols, chunk)
    ]
    ring = stage.shape[0]

    def piece_copy(i):
        _, hbm, lo, n = pieces[i]
        return pltpu.make_async_copy(hbm.at[lo:lo + n], stage.at[i % ring, 0:n], st_sems.at[i % ring])

    def unpack(layer, i):
        k, _, lo, n = pieces[i]
        slot = i % ring

        @pl.loop(0, n // 16)
        def _(j):
            r = pl.multiple_of(j * 16, 16)
            pair = pltpu.einshape('alk->lak', stage[slot, pl.ds(r, 16)])
            w_buf[k, here.c, pl.ds(pl.multiple_of(lo + r, 16), 16), :] = pair[layer]
        if n % 16:
            r = n - n % 16
            pair = pltpu.einshape('alk->lak', stage[slot, r:n])
            w_buf[k, here.c, lo + r:lo + n, :] = pair[layer]

    def share(layer, i):
        piece_copy(i).wait()
        unpack(layer, i)
        if i + ring < len(pieces):
            piece_copy(i + ring).start()
        elif layer + 1 < n_layers:
            piece_copy(i + ring - len(pieces)).start()
        k = pieces[i][0]
        if i + 1 == len(pieces) or pieces[i + 1][0] != k:
            if layer and k == 0:
                pl.semaphore_wait(credit, 1)
            mine = w_buf.at[k, here.c]
            swaps.append(_send(mine, mine, ws_sems, k, partner))

    def exchange(src, dst, sems, i, k):
        return pltpu.make_async_remote_copy(
            src_ref=src.at[peers[k]['tp'], i], dst_ref=dst.at[here.tp, i],
            send_sem=sems.at[0, 3 * i + k], recv_sem=sems.at[1, 3 * i + k],
            device_id=peers[k], device_id_type=MESH,
        )

    q_copy = functools.partial(exchange, q_send, q_recv, q_sems)
    o_copy = functools.partial(exchange, o_send, o_all, o_sems)

    for n in range(3):
        wq_copy(0, n).start()
    for i in range(2):
        cache_copy(0, i).start()
    for i in range(ring):
        piece_copy(i).start()
    wo_copy(0).start()
    _greet(cube + [partner])

    for layer in range(n_layers):
        last = layer + 1 == n_layers
        x_all = x_ref if layer == 0 else h_all

        for t in range(4):
            h_buf[t * rows:(t + 1) * rows, :] = _norm(x_all[t], an_ref[layer:layer + 1, :])
        for n in range(3):
            wq_copy(layer, n).wait()
            part = slice(n * q_width, (n + 1) * q_width)
            q = jnp.dot(h_buf[...], wq_buf[:, part], preferred_element_type=F32).astype(BF16)
            q_send[:, :, :, part] = q.reshape(4, units, unit, q_width)
        for i in range(units):
            for k in range(3):
                q_copy(i, k).start()
        if not last:
            for n in range(3):
                wq_copy(layer + 1, n).start()
        q_recv[here.tp] = q_send[here.tp]

        if layer == 0:
            for i in range(len(pieces)):
                share(0, i)

        @pl.loop(0, units)
        def _(i):
            slot = lax.rem(i, 2)
            for k in range(3):
                q_copy(i, k).wait_recv()
            for h in range(heads):
                q = q_recv[:, i, :, h * kv:(h + 1) * kv]
                q_att[:, 4 * h:4 * h + 4, :] = pltpu.einshape('tbk->btk', q)
            cache_copy(layer, i).wait()
            for lo in range(0, unit, 4):
                scores = [
                    jnp.dot(q_att[k], c_buf[slot, k], preferred_element_type=F32)
                    for k in range(lo, lo + 4)
                ]
                probs = []
                for k, s in enumerate(scores, lo):
                    keep = lax.broadcasted_iota(jnp.int32, s.shape, 1) < len_ref[here.tp * rows + i * unit + k]
                    s = jnp.where(keep, s * SCALE, -jnp.inf)
                    e = jnp.exp(s - jnp.max(s, axis=-1, keepdims=True))
                    probs.append((e / jnp.sum(e, axis=-1, keepdims=True)).astype(BF16))
                for k, p in enumerate(probs, lo):
                    o = lax.dot_general(
                        p, c_buf[slot, k, 0:LAT, :], (((1,), (1,)), ((), ())), preferred_element_type=F32
                    )
                    for j in range(LAT // 128):
                        o_rows[j, k * 16:(k + 1) * 16, :] = o[:, j * 128:(j + 1) * 128]
            for h in range(heads):
                for t in range(4):
                    for j in range(LAT // 128):
                        part = slice(j * 128, (j + 1) * 128)
                        o_send[t, i, h, :, part] = o_rows[j, pl.ds(4 * h + t, unit, stride=16), :].astype(BF16)
            for k in range(3):
                o_copy(i, k).start()
            o_all[here.tp, i] = o_send[here.tp, i]

            @pl.when(i + 2 < units)
            def _():
                cache_copy(layer, i + 2).start()
        if not last:
            for i in range(2):
                cache_copy(layer + 1, i).start()
        wo_copy(layer).wait()
        for i in range(units):
            for k in range(3):
                o_copy(i, k).wait_recv()

        wide = p_buf.shape[-1]
        lhs = jnp.concatenate([o_all[:, :, h].reshape(4 * rows, LAT) for h in range(heads)], axis=1)
        attn = Halving(here, ('z', 'y'), p_buf, (pr1, pr2), p_sems, TP_ORDERS)
        for n in range(len(TP_ORDERS)):
            part = slice(n * wide, (n + 1) * wide)
            p_buf[n] = jnp.dot(lhs, wo_buf[:, part], preferred_element_type=F32).reshape(p_buf.shape[1:])
            attn.send(n, 0)
        if not last:
            wo_copy(layer + 1).start()
        for n in range(len(TP_ORDERS)):
            attn.add(n, 0)
            attn.send(n, 1)
        x_mine = x_ref[here.tp] if layer == 0 else x_buf[...]
        g_copies = []
        for n in range(len(TP_ORDERS)):
            part = slice(n * wide, (n + 1) * wide)
            total = attn.add(n, 1).astype(BF16)
            x_part = (x_mine[:, part].astype(F32) + total.astype(F32)).astype(BF16)
            x_buf[:, part] = x_part
            g_all[here.x, here.tp, :, part] = x_part
            mine = g_all.at[here.x, here.tp, :, part]
            g_copies.append([_send(mine, mine, g_sems, 7 * n + k, device) for k, device in enumerate(cube)])

        def g_norm(x, t):
            at = pl.multiple_of((4 * x + t) * rows, rows)
            g_buf[pl.ds(at, rows), :] = _norm(g_all[x, t], fn_ref[layer:layer + 1, :])

        g_norm(here.x, here.tp)
        for copy in swaps:
            copy.wait()
        swaps.clear()
        for k, device in enumerate(cube):
            for copies in g_copies:
                copies[k].wait_recv()
            g_norm(lax.div(device['dp'], 2), device['tp'])

        @pl.loop(0, 2)
        def _(s):
            for lo in range(0, cols, 256):
                part = slice(lo, min(lo + 256, cols))
                u, v = (
                    lax.dot_general(
                        w_buf[k, s, part, :], g_buf[...], (((1,), (1,)), ((), ())), preferred_element_type=F32
                    ) for k in range(2)
                )
                a_buf[s, :, part] = (u * jax.nn.sigmoid(u) * v).T.astype(BF16)

        ffn = Halving(here, ('x', 'z', 'y'), y_buf, (yr1, yr2, yr3), y_sems, CUBE_ORDERS)
        for n in range(chunks):
            part = slice(n * width, (n + 1) * width)
            y = jnp.dot(a_buf[0], w_buf[2, 0, :, part], preferred_element_type=F32)
            y += jnp.dot(a_buf[1], w_buf[2, 1, :, part], preferred_element_type=F32)
            y_buf[n] = y.reshape(y_buf.shape[1:])
            ffn.send(n, 0)
        if not last:
            pl.semaphore_signal(credit, inc=1, device_id=partner, device_id_type=MESH)
        for phase in range(2):
            for n in range(chunks):
                ffn.add(n, phase)
                ffn.send(n, phase + 1)
                if not last and phase * chunks + n < len(pieces):
                    share(layer + 1, phase * chunks + n)
        h_copies = []
        for n in range(chunks):
            part = slice(n * width, (n + 1) * width)
            total = ffn.add(n, 2).astype(BF16)
            x_part = (x_buf[:, part].astype(F32) + total.astype(F32)).astype(BF16)
            x_buf[:, part] = x_part
            h_all[here.tp, :, part] = x_part
            mine = h_all.at[here.tp, :, part]
            h_copies += [_send(mine, mine, h_sems, 3 * n + k, peer) for k, peer in enumerate(peers)]

        for copy in h_copies:
            copy.wait_recv()
        attn.finish()
        ffn.finish()
        for copy in h_copies + [copy for copies in g_copies for copy in copies]:
            copy.wait_send()
        for i in range(units):
            for k in range(3):
                q_copy(i, k).wait_send()
                o_copy(i, k).wait_send()
    out_ref[...] = h_all[...]


VM = pl.BlockSpec(memory_space=pltpu.VMEM)
SM = pl.BlockSpec(memory_space=pltpu.SMEM)
ANY = pl.BlockSpec(memory_space=pl.ANY)
DMA = pltpu.SemaphoreType.DMA


def solution(mesh):
    def body(x, lengths, cache, attn_norm, ffn_norm, wq, wo, w1, w3, w2):
        nb, d = x.shape
        s_len, kv = cache.shape[2:]
        heads = wq.shape[2] // kv
        rows = nb // 4
        cols = w1.shape[2]
        unit = 8
        q_shape = (4, rows // unit, unit, heads * kv)
        scratch = [
            pltpu.VMEM(wq.shape[1:], BF16),
            pltpu.VMEM(wo.shape[1:], BF16),
            pltpu.VMEM((3, 2, cols, d), BF16),
            pltpu.VMEM((2, 176, 2, d), BF16),
            pltpu.VMEM((2, unit, kv, s_len), BF16),
            pltpu.VMEM((nb, d), BF16),
            pltpu.VMEM(q_shape, BF16),
            pltpu.VMEM(q_shape, BF16),
            pltpu.VMEM((unit, 4 * heads, kv), BF16),
            pltpu.VMEM((LAT // 128, unit * 4 * heads, 128), F32),
            pltpu.VMEM((4, rows // unit, heads, unit, LAT), BF16),
            pltpu.VMEM((4, rows // unit, heads, unit, LAT), BF16),
            pltpu.VMEM((4, 2, 2, rows, d // 4), F32),
            pltpu.VMEM((4, 2, rows, d // 4), F32),
            pltpu.VMEM((4, rows, d // 4), F32),
            pltpu.VMEM((rows, d), BF16),
            pltpu.VMEM((2, 4, rows, d), BF16),
            pltpu.VMEM((8 * rows, d), BF16),
            pltpu.VMEM((2, 8 * rows, cols), BF16),
            pltpu.VMEM((8, 2, 2, 2, rows, d // 8), F32),
            pltpu.VMEM((8, 2, 2, rows, d // 8), F32),
            pltpu.VMEM((8, 2, rows, d // 8), F32),
            pltpu.VMEM((8, rows, d // 8), F32),
            pltpu.VMEM((4, rows, d), BF16),
            DMA((3,)),
            DMA((1,)),
            DMA((2,)),
            DMA((2, 3)),
            DMA((2,)),
            DMA((2, 12)),
            DMA((2, 12)),
            DMA((2, 8)),
            DMA((2, 28)),
            DMA((2, 24)),
            DMA((2, 24)),
            pltpu.SemaphoreType.REGULAR,
        ]
        out = pl.pallas_call(
            _kernel,
            out_shape=jax.ShapeDtypeStruct((4, rows, d), BF16),
            in_specs=[SM, VM, VM, VM] + [ANY] * 6,
            out_specs=VM,
            scratch_shapes=scratch,
            compiler_params=pltpu.CompilerParams(
                collective_id=0, has_side_effects=True, vmem_limit_bytes=VMEM_LIMIT,
            ),
            name='two_layers',
        )(
            lengths, x.reshape(4, rows, d), attn_norm, ffn_norm, cache.transpose(0, 1, 3, 2), wq, wo,
            w1.transpose(2, 0, 1), w3.transpose(2, 0, 1), w2.transpose(1, 0, 2),
        )
        return out.reshape(nb, d)

    in_specs = (
        P('dp', None),
        P('dp'),
        P(None, 'dp', None, None),
        P(None, None),
        P(None, None),
        P(None, None, 'tp'),
        P(None, 'tp', None),
        P(None, None, ('dp', 'tp')),
        P(None, None, ('dp', 'tp')),
        P(None, ('dp', 'tp'), None),
    )
    return jax.shard_map(body, mesh=mesh, in_specs=in_specs, out_specs=P('dp', None), check_vma=False)
```

```python
import functools

import jax
import jax.numpy as jnp
from jax import lax
from jax.experimental import pallas as pl
from jax.experimental.pallas import tpu as pltpu
from jax.sharding import PartitionSpec as P

MESH = pl.DeviceIdType.MESH
F32 = jnp.float32
BF16 = jnp.bfloat16
LAT = 512
EPS = 1e-6
SCALE = 192 ** -0.5
VMEM_LIMIT = 64 * 1024 * 1024 - 65536

TP_ORDERS = (('z', 'y'), ('y', 'z')) * 2
CUBE_ORDERS = (
    ('x', 'y', 'z'), ('y', 'z', 'x'), ('z', 'x', 'y'),
    ('x', 'y', 'z'), ('y', 'z', 'x'), ('z', 'x', 'y'),
    ('x', 'y', 'z'), ('y', 'z', 'x'),
)
NEAR = ((1, 0, 0), (0, 1, 0), (0, 0, 1), (0, 1, 1), (1, 1, 0), (1, 0, 1), (1, 1, 1))
CROSSINGS = ((0, 1, 0), (0, 0, 1), (1, 0, 0), (1, 0, 0))
TP_PEERS = ((1, 0), (0, 1), (1, 1))


class Place:
    def __init__(self):
        self.tp, self.dp = lax.axis_index('tp'), lax.axis_index('dp')
        self.z, self.y = lax.div(self.tp, 2), lax.rem(self.tp, 2)
        self.x, self.c = lax.div(self.dp, 2), lax.rem(self.dp, 2)
        self.at = {'x': self.x, 'z': self.z, 'y': self.y}

    def other(self, dx=0, dz=0, dy=0, dc=0):
        x = 1 - self.x if dx else self.x
        z = 1 - self.z if dz else self.z
        y = 1 - self.y if dy else self.y
        c = 1 - self.c if dc else self.c
        return {'tp': 2 * z + y, 'dp': 2 * x + c}

    def along(self, axis):
        return self.other(**{'d' + axis: 1})


def _send(src, dst, sems, k, device):
    copy = pltpu.make_async_remote_copy(
        src_ref=src, dst_ref=dst, send_sem=sems.at[0, k], recv_sem=sems.at[1, k],
        device_id=device, device_id_type=MESH,
    )
    copy.start()
    return copy


def _norm(v, w):
    vf = v.astype(F32)
    r = lax.rsqrt(jnp.mean(vf * vf, axis=-1, keepdims=True) + EPS)
    return (vf * r * w.astype(F32)).astype(BF16)


def _greet(devices):
    barrier = pltpu.get_barrier_semaphore()
    for device in devices:
        pl.semaphore_signal(barrier, inc=1, device_id=device, device_id_type=MESH)
    return functools.partial(pl.semaphore_wait, barrier, len(devices))


def _meet(a, b):
    return any(p and q for p, q in zip(a, b))


class Halving:
    def __init__(self, here, axes, buf, recvs, sems, orders):
        self.here, self.axes, self.buf, self.recvs, self.sems, self.orders = here, axes, buf, recvs, sems, orders
        self.copies = {}

    def _view(self, chunk, phase, flip):
        index = [slice(None)] * len(self.axes)
        for p, axis in enumerate(self.orders[chunk][: phase + 1]):
            mine = self.here.at[axis]
            index[self.axes.index(axis)] = 1 - mine if (flip and p == phase) else mine
        return (chunk, *index)

    def send(self, chunk, phase):
        axis = self.orders[chunk][phase]
        self.copies[chunk, phase] = _send(
            self.buf.at[self._view(chunk, phase, True)], self.recvs[phase].at[chunk],
            self.sems, phase * len(self.orders) + chunk, self.here.along(axis),
        )

    def add(self, chunk, phase):
        self.copies[chunk, phase].wait_recv()
        view = self._view(chunk, phase, False)
        total = self.buf[view] + self.recvs[phase][chunk]
        if phase + 1 < len(self.axes):
            self.buf[view] = total
        return total

    def finish(self):
        for copy in self.copies.values():
            copy.wait_send()


def _kernel(
    len_ref, x_ref, an_ref, fn_ref, cache_hbm, wq_hbm, wo_hbm, w1_hbm, w3_hbm, w2_hbm, out_ref,
    wq_buf, wo_buf, w_buf, stage, c_buf, h_buf, q_send, q_recv, q_att, o_rows, o_send, o_all,
    p_buf, pr1, pr2, x_buf, g_all, g_buf, a_buf, y_buf, yr1, yr2, yr3, h_all,
    wq_sems, wo_sem, st_sems, ws_sems, c_sems, q_sems, o_sems, p_sems, g_sems, y_sems, h_sems, credit,
):
    here = Place()
    n_layers = cache_hbm.shape[0]
    d = x_buf.shape[1]
    rows = x_buf.shape[0]
    unit = c_buf.shape[1]
    units = rows // unit
    cols = w_buf.shape[2]
    chunk = stage.shape[1]
    heads = o_send.shape[2]
    kv = c_buf.shape[2]
    q_width = q_send.shape[-1] // 3
    chunks = len(CUBE_ORDERS)
    width = d // chunks
    swaps = []
    partner = here.other(dc=1)
    peers = [here.other(dz=dz, dy=dy) for dz, dy in TP_PEERS]
    cube = [here.other(dx=dx, dz=dz, dy=dy) for dx, dz, dy in NEAR]

    def wq_copy(layer, n):
        part = slice(n * q_width, (n + 1) * q_width)
        return pltpu.make_async_copy(wq_hbm.at[layer, :, part], wq_buf.at[:, part], wq_sems.at[n])

    def wo_copy(layer):
        return pltpu.make_async_copy(wo_hbm.at[layer], wo_buf, wo_sem.at[0])

    def cache_copy(layer, i):
        slot = lax.rem(i, 2)
        return pltpu.make_async_copy(
            cache_hbm.at[layer, pl.ds(here.tp * rows + i * unit, unit)], c_buf.at[slot], c_sems.at[slot]
        )

    pieces = [
        (k, hbm, lo, min(chunk, cols - lo))
        for k, hbm in enumerate((w3_hbm, w1_hbm, w2_hbm)) for lo in range(0, cols, chunk)
    ]
    ring = stage.shape[0]

    def piece_copy(i):
        _, hbm, lo, n = pieces[i]
        return pltpu.make_async_copy(hbm.at[lo:lo + n], stage.at[i % ring, 0:n], st_sems.at[i % ring])

    def unpack(layer, i):
        k, _, lo, n = pieces[i]
        slot = i % ring

        @pl.loop(0, n // 16)
        def _(j):
            r = pl.multiple_of(j * 16, 16)
            pair = pltpu.einshape('alk->lak', stage[slot, pl.ds(r, 16)])
            w_buf[k, here.c, pl.ds(pl.multiple_of(lo + r, 16), 16), :] = pair[layer]
        if n % 16:
            r = n - n % 16
            pair = pltpu.einshape('alk->lak', stage[slot, r:n])
            w_buf[k, here.c, lo + r:lo + n, :] = pair[layer]

    def share(layer, i):
        piece_copy(i).wait()
        unpack(layer, i)
        if i + ring < len(pieces):
            piece_copy(i + ring).start()
        elif layer + 1 < n_layers:
            piece_copy(i + ring - len(pieces)).start()
        k = pieces[i][0]
        if i + 1 == len(pieces) or pieces[i + 1][0] != k:
            if layer and k == 0:
                pl.semaphore_wait(credit, 1)
            mine = w_buf.at[k, here.c]
            swaps.append(_send(mine, mine, ws_sems, k, partner))

    def exchange(src, dst, sems, i, k):
        return pltpu.make_async_remote_copy(
            src_ref=src.at[peers[k]['tp'], i], dst_ref=dst.at[here.tp, i],
            send_sem=sems.at[0, 3 * i + k], recv_sem=sems.at[1, 3 * i + k],
            device_id=peers[k], device_id_type=MESH,
        )

    q_copy = functools.partial(exchange, q_send, q_recv, q_sems)
    o_copy = functools.partial(exchange, o_send, o_all, o_sems)

    for n in range(3):
        wq_copy(0, n).start()
    for i in range(2):
        cache_copy(0, i).start()
    for i in range(ring):
        piece_copy(i).start()
    wo_copy(0).start()
    greeted = _greet(cube + [partner])

    for layer in range(n_layers):
        last = layer + 1 == n_layers
        x_all = x_ref if layer == 0 else h_all

        for t in range(4):
            h_buf[t * rows:(t + 1) * rows, :] = _norm(x_all[t], an_ref[layer:layer + 1, :])
        for n in range(3):
            wq_copy(layer, n).wait()
            part = slice(n * q_width, (n + 1) * q_width)
            q = jnp.dot(h_buf[...], wq_buf[:, part], preferred_element_type=F32).astype(BF16)
            q_send[:, :, :, part] = q.reshape(4, units, unit, q_width)
        if layer == 0:
            greeted()
        for i in range(units):
            for k in range(3):
                q_copy(i, k).start()
        if not last:
            for n in range(3):
                wq_copy(layer + 1, n).start()
        q_recv[here.tp] = q_send[here.tp]

        if layer == 0:
            for i in range(len(pieces)):
                share(0, i)

        @pl.loop(0, units)
        def _(i):
            slot = lax.rem(i, 2)
            for k in range(3):
                q_copy(i, k).wait_recv()
            for h in range(heads):
                q = q_recv[:, i, :, h * kv:(h + 1) * kv]
                q_att[:, 4 * h:4 * h + 4, :] = pltpu.einshape('tbk->btk', q)
            cache_copy(layer, i).wait()
            for lo in range(0, unit, 4):
                scores = [
                    jnp.dot(q_att[k], c_buf[slot, k], preferred_element_type=F32)
                    for k in range(lo, lo + 4)
                ]
                probs = []
                for k, s in enumerate(scores, lo):
                    keep = lax.broadcasted_iota(jnp.int32, s.shape, 1) < len_ref[here.tp * rows + i * unit + k]
                    s = jnp.where(keep, s * SCALE, -jnp.inf)
                    e = jnp.exp(s - jnp.max(s, axis=-1, keepdims=True))
                    probs.append((e / jnp.sum(e, axis=-1, keepdims=True)).astype(BF16))
                for k, p in enumerate(probs, lo):
                    o = lax.dot_general(
                        p, c_buf[slot, k, 0:LAT, :], (((1,), (1,)), ((), ())), preferred_element_type=F32
                    )
                    for j in range(LAT // 128):
                        o_rows[j, k * 16:(k + 1) * 16, :] = o[:, j * 128:(j + 1) * 128]
            for h in range(heads):
                for t in range(4):
                    for j in range(LAT // 128):
                        part = slice(j * 128, (j + 1) * 128)
                        o_send[t, i, h, :, part] = o_rows[j, pl.ds(4 * h + t, unit, stride=16), :].astype(BF16)
            for k in range(3):
                o_copy(i, k).start()
            o_all[here.tp, i] = o_send[here.tp, i]

            @pl.when(i + 2 < units)
            def _():
                cache_copy(layer, i + 2).start()
        if not last:
            for i in range(2):
                cache_copy(layer + 1, i).start()
        wo_copy(layer).wait()
        for i in range(units):
            for k in range(3):
                o_copy(i, k).wait_recv()

        wide = p_buf.shape[-1]
        lhs = jnp.concatenate([o_all[:, :, h].reshape(4 * rows, LAT) for h in range(heads)], axis=1)
        attn = Halving(here, ('z', 'y'), p_buf, (pr1, pr2), p_sems, TP_ORDERS)
        for n in range(len(TP_ORDERS)):
            part = slice(n * wide, (n + 1) * wide)
            p_buf[n] = jnp.dot(lhs, wo_buf[:, part], preferred_element_type=F32).reshape(p_buf.shape[1:])
            attn.send(n, 0)
        if not last:
            wo_copy(layer + 1).start()
        for n in range(len(TP_ORDERS)):
            attn.add(n, 0)
            attn.send(n, 1)
        x_mine = x_ref[here.tp] if layer == 0 else x_buf[...]
        g_copies = []

        def g_send(n, source, target, sem):
            device = here.other(*source)
            block = g_all.at[lax.div(device['dp'], 2), device['tp'], :, n * wide:(n + 1) * wide]
            return _send(block, block, g_sems, 7 * n + NEAR.index(sem), here.other(*target))

        for n in range(len(TP_ORDERS)):
            part = slice(n * wide, (n + 1) * wide)
            total = attn.add(n, 1).astype(BF16)
            x_part = (x_mine[:, part].astype(F32) + total.astype(F32)).astype(BF16)
            x_buf[:, part] = x_part
            g_all[here.x, here.tp, :, part] = x_part
            axis = CROSSINGS[n]
            sent = {}
            for offset in NEAR:
                if offset == axis or not _meet(offset, axis):
                    sent[offset] = g_send(n, (0, 0, 0), offset, offset)
            g_copies.append(sent)
        for n, sent in enumerate(g_copies):
            axis = CROSSINGS[n]
            for offset in NEAR:
                if not _meet(offset, axis):
                    sent[offset].wait_recv()
                    both = tuple(a + b for a, b in zip(offset, axis))
                    sent[both] = g_send(n, offset, axis, both)

        def g_norm(x, t):
            at = pl.multiple_of((4 * x + t) * rows, rows)
            g_buf[pl.ds(at, rows), :] = _norm(g_all[x, t], fn_ref[layer:layer + 1, :])

        g_norm(here.x, here.tp)
        for copy in swaps:
            copy.wait()
        swaps.clear()
        for offset, device in zip(NEAR, cube):
            for n, sent in enumerate(g_copies):
                if _meet(offset, CROSSINGS[n]):
                    sent[offset].wait_recv()
            g_norm(lax.div(device['dp'], 2), device['tp'])

        for sent in g_copies:
            for copy in sent.values():
                copy.wait_send()

        @pl.loop(0, 2)
        def _(s):
            for lo in range(0, cols, 256):
                part = slice(lo, min(lo + 256, cols))
                u, v = (
                    lax.dot_general(
                        w_buf[k, s, part, :], g_buf[...], (((1,), (1,)), ((), ())), preferred_element_type=F32
                    ) for k in range(2)
                )
                a_buf[s, :, part] = (u * jax.nn.sigmoid(u) * v).T.astype(BF16)

        ffn = Halving(here, ('x', 'z', 'y'), y_buf, (yr1, yr2, yr3), y_sems, CUBE_ORDERS)
        for n in range(chunks):
            part = slice(n * width, (n + 1) * width)
            y = jnp.dot(a_buf[0], w_buf[2, 0, :, part], preferred_element_type=F32)
            y += jnp.dot(a_buf[1], w_buf[2, 1, :, part], preferred_element_type=F32)
            y_buf[n] = y.reshape(y_buf.shape[1:])
            ffn.send(n, 0)
        if not last:
            pl.semaphore_signal(credit, inc=1, device_id=partner, device_id_type=MESH)
        for phase in range(2):
            for n in range(chunks):
                ffn.add(n, phase)
                ffn.send(n, phase + 1)
                if not last and phase * chunks + n < len(pieces):
                    share(layer + 1, phase * chunks + n)
        h_copies = []
        for n in range(chunks):
            part = slice(n * width, (n + 1) * width)
            total = ffn.add(n, 2).astype(BF16)
            x_part = (x_buf[:, part].astype(F32) + total.astype(F32)).astype(BF16)
            x_buf[:, part] = x_part
            h_all[here.tp, :, part] = x_part
            mine = h_all.at[here.tp, :, part]
            h_copies += [_send(mine, mine, h_sems, 3 * n + k, peer) for k, peer in enumerate(peers)]

        for copy in h_copies:
            copy.wait_recv()
        attn.finish()
        ffn.finish()
        for copy in h_copies:
            copy.wait_send()
        for i in range(units):
            for k in range(3):
                q_copy(i, k).wait_send()
                o_copy(i, k).wait_send()
    out_ref[...] = h_all[...]


VM = pl.BlockSpec(memory_space=pltpu.VMEM)
SM = pl.BlockSpec(memory_space=pltpu.SMEM)
ANY = pl.BlockSpec(memory_space=pl.ANY)
DMA = pltpu.SemaphoreType.DMA


def solution(mesh):
    def body(x, lengths, cache, attn_norm, ffn_norm, wq, wo, w1, w3, w2):
        nb, d = x.shape
        s_len, kv = cache.shape[2:]
        heads = wq.shape[2] // kv
        rows = nb // 4
        cols = w1.shape[2]
        unit = 8
        q_shape = (4, rows // unit, unit, heads * kv)
        scratch = [
            pltpu.VMEM(wq.shape[1:], BF16),
            pltpu.VMEM(wo.shape[1:], BF16),
            pltpu.VMEM((3, 2, cols, d), BF16),
            pltpu.VMEM((2, 176, 2, d), BF16),
            pltpu.VMEM((2, unit, kv, s_len), BF16),
            pltpu.VMEM((nb, d), BF16),
            pltpu.VMEM(q_shape, BF16),
            pltpu.VMEM(q_shape, BF16),
            pltpu.VMEM((unit, 4 * heads, kv), BF16),
            pltpu.VMEM((LAT // 128, unit * 4 * heads, 128), F32),
            pltpu.VMEM((4, rows // unit, heads, unit, LAT), BF16),
            pltpu.VMEM((4, rows // unit, heads, unit, LAT), BF16),
            pltpu.VMEM((4, 2, 2, rows, d // 4), F32),
            pltpu.VMEM((4, 2, rows, d // 4), F32),
            pltpu.VMEM((4, rows, d // 4), F32),
            pltpu.VMEM((rows, d), BF16),
            pltpu.VMEM((2, 4, rows, d), BF16),
            pltpu.VMEM((8 * rows, d), BF16),
            pltpu.VMEM((2, 8 * rows, cols), BF16),
            pltpu.VMEM((8, 2, 2, 2, rows, d // 8), F32),
            pltpu.VMEM((8, 2, 2, rows, d // 8), F32),
            pltpu.VMEM((8, 2, rows, d // 8), F32),
            pltpu.VMEM((8, rows, d // 8), F32),
            pltpu.VMEM((4, rows, d), BF16),
            DMA((3,)),
            DMA((1,)),
            DMA((2,)),
            DMA((2, 3)),
            DMA((2,)),
            DMA((2, 12)),
            DMA((2, 12)),
            DMA((2, 8)),
            DMA((2, 28)),
            DMA((2, 24)),
            DMA((2, 24)),
            pltpu.SemaphoreType.REGULAR,
        ]
        out = pl.pallas_call(
            _kernel,
            out_shape=jax.ShapeDtypeStruct((4, rows, d), BF16),
            in_specs=[SM, VM, VM, VM] + [ANY] * 6,
            out_specs=VM,
            scratch_shapes=scratch,
            compiler_params=pltpu.CompilerParams(
                collective_id=0, has_side_effects=True, vmem_limit_bytes=VMEM_LIMIT,
            ),
            name='two_layers',
        )(
            lengths, x.reshape(4, rows, d), attn_norm, ffn_norm, cache.transpose(0, 1, 3, 2), wq, wo,
            w1.transpose(2, 0, 1), w3.transpose(2, 0, 1), w2.transpose(1, 0, 2),
        )
        return out.reshape(nb, d)

    in_specs = (
        P('dp', None),
        P('dp'),
        P(None, 'dp', None, None),
        P(None, None),
        P(None, None),
        P(None, None, 'tp'),
        P(None, 'tp', None),
        P(None, None, ('dp', 'tp')),
        P(None, None, ('dp', 'tp')),
        P(None, ('dp', 'tp'), None),
    )
    return jax.shard_map(body, mesh=mesh, in_specs=in_specs, out_specs=P('dp', None), check_vma=False)
```

```python
import functools

import jax
import jax.numpy as jnp
from jax import lax
from jax.experimental import pallas as pl
from jax.experimental.pallas import tpu as pltpu
from jax.sharding import PartitionSpec as P

MESH = pl.DeviceIdType.MESH
F32 = jnp.float32
BF16 = jnp.bfloat16
LAT = 512
EPS = 1e-6
SCALE = 192 ** -0.5
VMEM_LIMIT = 64 * 1024 * 1024 - 65536

TP_ORDERS = (('z', 'y'), ('y', 'z')) * 4
CUBE_ORDERS = (
    ('x', 'y', 'z'), ('y', 'z', 'x'), ('z', 'x', 'y'),
    ('x', 'y', 'z'), ('y', 'z', 'x'), ('z', 'x', 'y'),
    ('x', 'y', 'z'), ('y', 'z', 'x'),
)
NEAR = ((1, 0, 0), (0, 1, 0), (0, 0, 1), (0, 1, 1), (1, 1, 0), (1, 0, 1), (1, 1, 1))
CROSSINGS = ((0, 1, 0), (0, 0, 1), (1, 0, 0), (1, 0, 0)) * 2
TP_PEERS = ((1, 0), (0, 1), (1, 1))


class Place:
    def __init__(self):
        self.tp, self.dp = lax.axis_index('tp'), lax.axis_index('dp')
        self.z, self.y = lax.div(self.tp, 2), lax.rem(self.tp, 2)
        self.x, self.c = lax.div(self.dp, 2), lax.rem(self.dp, 2)
        self.at = {'x': self.x, 'z': self.z, 'y': self.y}

    def other(self, dx=0, dz=0, dy=0, dc=0):
        x = 1 - self.x if dx else self.x
        z = 1 - self.z if dz else self.z
        y = 1 - self.y if dy else self.y
        c = 1 - self.c if dc else self.c
        return {'tp': 2 * z + y, 'dp': 2 * x + c}

    def along(self, axis):
        return self.other(**{'d' + axis: 1})


def _send(src, dst, sems, k, device):
    copy = pltpu.make_async_remote_copy(
        src_ref=src, dst_ref=dst, send_sem=sems.at[0, k], recv_sem=sems.at[1, k],
        device_id=device, device_id_type=MESH,
    )
    copy.start()
    return copy


def _norm(v, w):
    vf = v.astype(F32)
    r = lax.rsqrt(jnp.mean(vf * vf, axis=-1, keepdims=True) + EPS)
    return (vf * r * w.astype(F32)).astype(BF16)


def _greet(devices):
    barrier = pltpu.get_barrier_semaphore()
    for device in devices:
        pl.semaphore_signal(barrier, inc=1, device_id=device, device_id_type=MESH)
    return functools.partial(pl.semaphore_wait, barrier, len(devices))


def _meet(a, b):
    return any(p and q for p, q in zip(a, b))


class Halving:
    def __init__(self, here, axes, buf, recvs, sems, orders):
        self.here, self.axes, self.buf, self.recvs, self.sems, self.orders = here, axes, buf, recvs, sems, orders
        self.copies = {}

    def _view(self, chunk, phase, flip):
        index = [slice(None)] * len(self.axes)
        for p, axis in enumerate(self.orders[chunk][: phase + 1]):
            mine = self.here.at[axis]
            index[self.axes.index(axis)] = 1 - mine if (flip and p == phase) else mine
        return (chunk, *index)

    def send(self, chunk, phase):
        axis = self.orders[chunk][phase]
        self.copies[chunk, phase] = _send(
            self.buf.at[self._view(chunk, phase, True)], self.recvs[phase].at[chunk],
            self.sems, phase * len(self.orders) + chunk, self.here.along(axis),
        )

    def add(self, chunk, phase):
        self.copies[chunk, phase].wait_recv()
        view = self._view(chunk, phase, False)
        total = self.buf[view] + self.recvs[phase][chunk]
        if phase + 1 < len(self.axes):
            self.buf[view] = total
        return total

    def finish(self):
        for copy in self.copies.values():
            copy.wait_send()


def _kernel(
    len_ref, x_ref, an_ref, fn_ref, cache_hbm, wq_hbm, wo_hbm, w1_hbm, w3_hbm, w2_hbm, out_ref,
    wq_buf, wo_buf, w_buf, stage, c_buf, h_buf, q_send, q_recv, q_att, o_rows, o_send, o_all,
    p_buf, pr1, pr2, x_buf, g_all, g_buf, a_buf, y_buf, yr1, yr2, yr3, h_all,
    wq_sems, wo_sem, st_sems, ws_sems, c_sems, q_sems, o_sems, p_sems, g_sems, y_sems, h_sems, credit,
):
    here = Place()
    n_layers = cache_hbm.shape[0]
    d = x_buf.shape[1]
    rows = x_buf.shape[0]
    unit = c_buf.shape[1]
    units = rows // unit
    cols = w_buf.shape[2]
    chunk = stage.shape[1]
    heads = o_send.shape[2]
    kv = c_buf.shape[2]
    q_width = q_send.shape[-1] // 3
    chunks = len(CUBE_ORDERS)
    width = d // chunks
    swaps, h_copies = [], []
    partner = here.other(dc=1)
    peers = [here.other(dz=dz, dy=dy) for dz, dy in TP_PEERS]
    cube = [here.other(dx=dx, dz=dz, dy=dy) for dx, dz, dy in NEAR]

    def wq_copy(layer, n):
        part = slice(n * q_width, (n + 1) * q_width)
        return pltpu.make_async_copy(wq_hbm.at[layer, :, part], wq_buf.at[:, part], wq_sems.at[n])

    def wo_copy(layer):
        return pltpu.make_async_copy(wo_hbm.at[layer], wo_buf, wo_sem.at[0])

    def cache_copy(layer, i):
        slot = lax.rem(i, 2)
        return pltpu.make_async_copy(
            cache_hbm.at[layer, pl.ds(here.tp * rows + i * unit, unit)], c_buf.at[slot], c_sems.at[slot]
        )

    pieces = [
        (k, hbm, lo, min(chunk, cols - lo))
        for k, hbm in enumerate((w3_hbm, w1_hbm, w2_hbm)) for lo in range(0, cols, chunk)
    ]
    ring = stage.shape[0]

    def piece_copy(i):
        _, hbm, lo, n = pieces[i]
        return pltpu.make_async_copy(hbm.at[lo:lo + n], stage.at[i % ring, 0:n], st_sems.at[i % ring])

    def unpack(layer, i):
        k, _, lo, n = pieces[i]
        slot = i % ring

        @pl.loop(0, n // 16)
        def _(j):
            r = pl.multiple_of(j * 16, 16)
            pair = pltpu.einshape('alk->lak', stage[slot, pl.ds(r, 16)])
            w_buf[k, here.c, pl.ds(pl.multiple_of(lo + r, 16), 16), :] = pair[layer]
        if n % 16:
            r = n - n % 16
            pair = pltpu.einshape('alk->lak', stage[slot, r:n])
            w_buf[k, here.c, lo + r:lo + n, :] = pair[layer]

    def share(layer, i):
        piece_copy(i).wait()
        unpack(layer, i)
        if i + ring < len(pieces):
            piece_copy(i + ring).start()
        elif layer + 1 < n_layers:
            piece_copy(i + ring - len(pieces)).start()
        k = pieces[i][0]
        if i + 1 == len(pieces) or pieces[i + 1][0] != k:
            if layer and k == 0:
                pl.semaphore_wait(credit, 1)
            mine = w_buf.at[k, here.c]
            swaps.append(_send(mine, mine, ws_sems, k, partner))

    def exchange(src, dst, sems, i, k):
        return pltpu.make_async_remote_copy(
            src_ref=src.at[peers[k]['tp'], i], dst_ref=dst.at[here.tp, i],
            send_sem=sems.at[0, 3 * i + k], recv_sem=sems.at[1, 3 * i + k],
            device_id=peers[k], device_id_type=MESH,
        )

    q_copy = functools.partial(exchange, q_send, q_recv, q_sems)
    def q_head(n, k):
        part = slice(n * q_width, (n + 1) * q_width)
        return pltpu.make_async_remote_copy(
            src_ref=q_send.at[peers[k]['tp'], 0, :, part], dst_ref=q_recv.at[here.tp, 0, :, part],
            send_sem=q_sems.at[0, 3 * units + 3 * n + k], recv_sem=q_sems.at[1, 3 * units + 3 * n + k],
            device_id=peers[k], device_id_type=MESH,
        )

    o_copy = functools.partial(exchange, o_send, o_all, o_sems)

    for n in range(3):
        wq_copy(0, n).start()
    for i in range(2):
        cache_copy(0, i).start()
    for i in range(ring):
        piece_copy(i).start()
    wo_copy(0).start()
    greeted = _greet(cube + [partner])

    for layer in range(n_layers):
        last = layer + 1 == n_layers
        x_all = x_ref if layer == 0 else h_all

        def h_norm(t):
            at = pl.multiple_of(t * rows, rows)
            h_buf[pl.ds(at, rows), :] = _norm(x_all[t], an_ref[layer:layer + 1, :])

        h_norm(here.tp)
        for k, peer in enumerate(peers):
            for copy in h_copies[k::3]:
                copy.wait_recv()
            h_norm(peer['tp'])
        for n in range(3):
            wq_copy(layer, n).wait()
            part = slice(n * q_width, (n + 1) * q_width)
            q = jnp.dot(h_buf[...], wq_buf[:, part], preferred_element_type=F32).astype(BF16)
            q_send[:, :, :, part] = q.reshape(4, units, unit, q_width)
            if layer == 0 and n == 0:
                greeted()
            for k in range(3):
                q_head(n, k).start()
        for i in range(1, units):
            for k in range(3):
                q_copy(i, k).start()
        if not last:
            for n in range(3):
                wq_copy(layer + 1, n).start()
        q_recv[here.tp] = q_send[here.tp]

        if layer == 0:
            for i in range(len(pieces)):
                share(0, i)

        for n in range(3):
            for k in range(3):
                q_head(n, k).wait_recv()

        @pl.loop(0, units)
        def _(i):
            slot = lax.rem(i, 2)
            @pl.when(i > 0)
            def _():
                for k in range(3):
                    q_copy(i, k).wait_recv()
            for h in range(heads):
                q = q_recv[:, i, :, h * kv:(h + 1) * kv]
                q_att[:, 4 * h:4 * h + 4, :] = pltpu.einshape('tbk->btk', q)
            cache_copy(layer, i).wait()
            for lo in range(0, unit, 4):
                scores = [
                    jnp.dot(q_att[k], c_buf[slot, k], preferred_element_type=F32)
                    for k in range(lo, lo + 4)
                ]
                probs = []
                for k, s in enumerate(scores, lo):
                    keep = lax.broadcasted_iota(jnp.int32, s.shape, 1) < len_ref[here.tp * rows + i * unit + k]
                    s = jnp.where(keep, s * SCALE, -jnp.inf)
                    e = jnp.exp(s - jnp.max(s, axis=-1, keepdims=True))
                    probs.append((e / jnp.sum(e, axis=-1, keepdims=True)).astype(BF16))
                for k, p in enumerate(probs, lo):
                    o = lax.dot_general(
                        p, c_buf[slot, k, 0:LAT, :], (((1,), (1,)), ((), ())), preferred_element_type=F32
                    )
                    for j in range(LAT // 128):
                        o_rows[j, k * 16:(k + 1) * 16, :] = o[:, j * 128:(j + 1) * 128]
            for h in range(heads):
                for t in range(4):
                    for j in range(LAT // 128):
                        part = slice(j * 128, (j + 1) * 128)
                        o_send[t, i, h, :, part] = o_rows[j, pl.ds(4 * h + t, unit, stride=16), :].astype(BF16)
            for k in range(3):
                o_copy(i, k).start()
            o_all[here.tp, i] = o_send[here.tp, i]

            @pl.when(i + 2 < units)
            def _():
                cache_copy(layer, i + 2).start()
        if not last:
            for i in range(2):
                cache_copy(layer + 1, i).start()
        wo_copy(layer).wait()
        for i in range(units):
            for k in range(3):
                o_copy(i, k).wait_recv()

        wide = p_buf.shape[-1]
        lhs = jnp.concatenate([o_all[:, :, h].reshape(4 * rows, LAT) for h in range(heads)], axis=1)
        attn = Halving(here, ('z', 'y'), p_buf, (pr1, pr2), p_sems, TP_ORDERS)
        for n in range(0, len(TP_ORDERS), 2):
            y = jnp.dot(lhs, wo_buf[:, n * wide:(n + 2) * wide], preferred_element_type=F32)
            for k in range(2):
                p_buf[n + k] = y[:, k * wide:(k + 1) * wide].reshape(p_buf.shape[1:])
                attn.send(n + k, 0)
        if not last:
            wo_copy(layer + 1).start()
        for n in range(len(TP_ORDERS)):
            attn.add(n, 0)
            attn.send(n, 1)
        x_mine = x_ref[here.tp] if layer == 0 else x_buf[...]
        g_copies = []

        def g_send(n, source, target, sem):
            device = here.other(*source)
            block = g_all.at[lax.div(device['dp'], 2), device['tp'], :, n * wide:(n + 1) * wide]
            return _send(block, block, g_sems, 7 * n + NEAR.index(sem), here.other(*target))

        for n in range(len(TP_ORDERS)):
            part = slice(n * wide, (n + 1) * wide)
            total = attn.add(n, 1).astype(BF16)
            x_part = (x_mine[:, part].astype(F32) + total.astype(F32)).astype(BF16)
            x_buf[:, part] = x_part
            g_all[here.x, here.tp, :, part] = x_part
            axis = CROSSINGS[n]
            sent = {}
            for offset in NEAR:
                if offset == axis or not _meet(offset, axis):
                    sent[offset] = g_send(n, (0, 0, 0), offset, offset)
            g_copies.append(sent)
        for n, sent in enumerate(g_copies):
            axis = CROSSINGS[n]
            for offset in NEAR:
                if not _meet(offset, axis):
                    sent[offset].wait_recv()
                    both = tuple(a + b for a, b in zip(offset, axis))
                    sent[both] = g_send(n, offset, axis, both)

        def g_norm(x, t):
            at = pl.multiple_of((4 * x + t) * rows, rows)
            g_buf[pl.ds(at, rows), :] = _norm(g_all[x, t], fn_ref[layer:layer + 1, :])

        g_norm(here.x, here.tp)
        for copy in swaps:
            copy.wait()
        swaps.clear()
        for offset, device in zip(NEAR, cube):
            for n, sent in enumerate(g_copies):
                if _meet(offset, CROSSINGS[n]):
                    sent[offset].wait_recv()
            g_norm(lax.div(device['dp'], 2), device['tp'])

        for sent in g_copies:
            for copy in sent.values():
                copy.wait_send()

        @pl.loop(0, 2)
        def _(s):
            for lo in range(0, cols, 256):
                part = slice(lo, min(lo + 256, cols))
                u, v = (
                    lax.dot_general(
                        w_buf[k, s, part, :], g_buf[...], (((1,), (1,)), ((), ())), preferred_element_type=F32
                    ) for k in range(2)
                )
                a_buf[s, :, part] = (u * jax.nn.sigmoid(u) * v).T.astype(BF16)

        ffn = Halving(here, ('x', 'z', 'y'), y_buf, (yr1, yr2, yr3), y_sems, CUBE_ORDERS)
        for n in range(chunks):
            part = slice(n * width, (n + 1) * width)
            y = jnp.dot(a_buf[0], w_buf[2, 0, :, part], preferred_element_type=F32)
            y += jnp.dot(a_buf[1], w_buf[2, 1, :, part], preferred_element_type=F32)
            y_buf[n] = y.reshape(y_buf.shape[1:])
            ffn.send(n, 0)
        if not last:
            pl.semaphore_signal(credit, inc=1, device_id=partner, device_id_type=MESH)
        for phase in range(2):
            for n in range(chunks):
                ffn.add(n, phase)
                ffn.send(n, phase + 1)
                if not last and phase * chunks + n < len(pieces):
                    share(layer + 1, phase * chunks + n)
        h_copies = []
        for n in range(chunks):
            part = slice(n * width, (n + 1) * width)
            total = ffn.add(n, 2).astype(BF16)
            x_part = (x_buf[:, part].astype(F32) + total.astype(F32)).astype(BF16)
            x_buf[:, part] = x_part
            h_all[here.tp, :, part] = x_part
            mine = h_all.at[here.tp, :, part]
            h_copies += [_send(mine, mine, h_sems, 3 * n + k, peer) for k, peer in enumerate(peers)]

        attn.finish()
        ffn.finish()
        for copy in h_copies:
            copy.wait_send()
        for i in range(units):
            for k in range(3):
                (q_head(i - 1, k) if i else q_copy(units - 1, k)).wait_send()
                o_copy(i, k).wait_send()
        for i in range(1, units - 1):
            for k in range(3):
                q_copy(i, k).wait_send()
    for copy in h_copies:
        copy.wait_recv()
    out_ref[...] = h_all[...]


VM = pl.BlockSpec(memory_space=pltpu.VMEM)
SM = pl.BlockSpec(memory_space=pltpu.SMEM)
ANY = pl.BlockSpec(memory_space=pl.ANY)
DMA = pltpu.SemaphoreType.DMA


def solution(mesh):
    def body(x, lengths, cache, attn_norm, ffn_norm, wq, wo, w1, w3, w2):
        nb, d = x.shape
        s_len, kv = cache.shape[2:]
        heads = wq.shape[2] // kv
        rows = nb // 4
        cols = w1.shape[2]
        unit = 8
        q_shape = (4, rows // unit, unit, heads * kv)
        scratch = [
            pltpu.VMEM(wq.shape[1:], BF16),
            pltpu.VMEM(wo.shape[1:], BF16),
            pltpu.VMEM((3, 2, cols, d), BF16),
            pltpu.VMEM((2, 176, 2, d), BF16),
            pltpu.VMEM((2, unit, kv, s_len), BF16),
            pltpu.VMEM((nb, d), BF16),
            pltpu.VMEM(q_shape, BF16),
            pltpu.VMEM(q_shape, BF16),
            pltpu.VMEM((unit, 4 * heads, kv), BF16),
            pltpu.VMEM((LAT // 128, unit * 4 * heads, 128), F32),
            pltpu.VMEM((4, rows // unit, heads, unit, LAT), BF16),
            pltpu.VMEM((4, rows // unit, heads, unit, LAT), BF16),
            pltpu.VMEM((8, 2, 2, rows, d // 8), F32),
            pltpu.VMEM((8, 2, rows, d // 8), F32),
            pltpu.VMEM((8, rows, d // 8), F32),
            pltpu.VMEM((rows, d), BF16),
            pltpu.VMEM((2, 4, rows, d), BF16),
            pltpu.VMEM((8 * rows, d), BF16),
            pltpu.VMEM((2, 8 * rows, cols), BF16),
            pltpu.VMEM((8, 2, 2, 2, rows, d // 8), F32),
            pltpu.VMEM((8, 2, 2, rows, d // 8), F32),
            pltpu.VMEM((8, 2, rows, d // 8), F32),
            pltpu.VMEM((8, rows, d // 8), F32),
            pltpu.VMEM((4, rows, d), BF16),
            DMA((3,)),
            DMA((1,)),
            DMA((2,)),
            DMA((2, 3)),
            DMA((2,)),
            DMA((2, 21)),
            DMA((2, 12)),
            DMA((2, 16)),
            DMA((2, 56)),
            DMA((2, 24)),
            DMA((2, 24)),
            pltpu.SemaphoreType.REGULAR,
        ]
        out = pl.pallas_call(
            _kernel,
            out_shape=jax.ShapeDtypeStruct((4, rows, d), BF16),
            in_specs=[SM, VM, VM, VM] + [ANY] * 6,
            out_specs=VM,
            scratch_shapes=scratch,
            compiler_params=pltpu.CompilerParams(
                collective_id=0, has_side_effects=True, vmem_limit_bytes=VMEM_LIMIT,
            ),
            name='two_layers',
        )(
            lengths, x.reshape(4, rows, d), attn_norm, ffn_norm, cache.transpose(0, 1, 3, 2), wq, wo,
            w1.transpose(2, 0, 1), w3.transpose(2, 0, 1), w2.transpose(1, 0, 2),
        )
        return out.reshape(nb, d)

    in_specs = (
        P('dp', None),
        P('dp'),
        P(None, 'dp', None, None),
        P(None, None),
        P(None, None),
        P(None, None, 'tp'),
        P(None, 'tp', None),
        P(None, None, ('dp', 'tp')),
        P(None, None, ('dp', 'tp')),
        P(None, ('dp', 'tp'), None),
    )
    return jax.shard_map(body, mesh=mesh, in_specs=in_specs, out_specs=P('dp', None), check_vma=False)
```

```python
import functools

import jax
import jax.numpy as jnp
from jax import lax
from jax.experimental import pallas as pl
from jax.experimental.pallas import tpu as pltpu
from jax.sharding import PartitionSpec as P

MESH = pl.DeviceIdType.MESH
F32 = jnp.float32
BF16 = jnp.bfloat16
LAT = 512
EPS = 1e-6
SCALE = 192 ** -0.5
VMEM_LIMIT = 64 * 1024 * 1024 - 65536

TP_ORDERS = (('z', 'y'), ('y', 'z')) * 4
CUBE_ORDERS = (
    ('x', 'y', 'z'), ('y', 'z', 'x'), ('z', 'x', 'y'),
    ('x', 'y', 'z'), ('y', 'z', 'x'), ('z', 'x', 'y'),
    ('x', 'y', 'z'), ('y', 'z', 'x'),
)
NEAR = ((1, 0, 0), (0, 1, 0), (0, 0, 1), (0, 1, 1), (1, 1, 0), (1, 0, 1), (1, 1, 1))
CROSSINGS = ((0, 1, 0), (0, 0, 1), (1, 0, 0), (1, 0, 0)) * 2
TP_PEERS = ((1, 0), (0, 1), (1, 1))


class Place:
    def __init__(self):
        self.tp, self.dp = lax.axis_index('tp'), lax.axis_index('dp')
        self.z, self.y = lax.div(self.tp, 2), lax.rem(self.tp, 2)
        self.x, self.c = lax.div(self.dp, 2), lax.rem(self.dp, 2)
        self.at = {'x': self.x, 'z': self.z, 'y': self.y}

    def other(self, dx=0, dz=0, dy=0, dc=0):
        x = 1 - self.x if dx else self.x
        z = 1 - self.z if dz else self.z
        y = 1 - self.y if dy else self.y
        c = 1 - self.c if dc else self.c
        return {'tp': 2 * z + y, 'dp': 2 * x + c}

    def along(self, axis):
        return self.other(**{'d' + axis: 1})


def _send(src, dst, sems, k, device):
    copy = pltpu.make_async_remote_copy(
        src_ref=src, dst_ref=dst, send_sem=sems.at[0, k], recv_sem=sems.at[1, k],
        device_id=device, device_id_type=MESH,
    )
    copy.start()
    return copy


def _norm(v, w):
    vf = v.astype(F32)
    r = lax.rsqrt(jnp.mean(vf * vf, axis=-1, keepdims=True) + EPS)
    return (vf * r * w.astype(F32)).astype(BF16)


def _greet(devices):
    barrier = pltpu.get_barrier_semaphore()
    for device in devices:
        pl.semaphore_signal(barrier, inc=1, device_id=device, device_id_type=MESH)
    return functools.partial(pl.semaphore_wait, barrier, len(devices))


def _meet(a, b):
    return any(p and q for p, q in zip(a, b))


class Halving:
    def __init__(self, here, axes, buf, recvs, sems, orders):
        self.here, self.axes, self.buf, self.recvs, self.sems, self.orders = here, axes, buf, recvs, sems, orders
        self.copies = {}

    def _view(self, chunk, phase, flip):
        index = [slice(None)] * len(self.axes)
        for p, axis in enumerate(self.orders[chunk][: phase + 1]):
            mine = self.here.at[axis]
            index[self.axes.index(axis)] = 1 - mine if (flip and p == phase) else mine
        return (chunk, *index)

    def send(self, chunk, phase):
        axis = self.orders[chunk][phase]
        self.copies[chunk, phase] = _send(
            self.buf.at[self._view(chunk, phase, True)], self.recvs[phase].at[chunk],
            self.sems, phase * len(self.orders) + chunk, self.here.along(axis),
        )

    def add(self, chunk, phase):
        self.copies[chunk, phase].wait_recv()
        view = self._view(chunk, phase, False)
        total = self.buf[view] + self.recvs[phase][chunk]
        if phase + 1 < len(self.axes):
            self.buf[view] = total
        return total

    def finish(self):
        for copy in self.copies.values():
            copy.wait_send()


def _kernel(
    len_ref, x_ref, an_ref, fn_ref, cache_hbm, wq_hbm, wo_hbm, w1_hbm, w3_hbm, w2_hbm, out_ref,
    wq_buf, wo_buf, w_buf, stage, c_buf, h_buf, q_send, q_recv, q_att, o_rows, o_send, o_all,
    p_buf, pr1, pr2, x_buf, g_all, g_buf, a_buf, y_buf, yr1, yr2, yr3, h_all,
    wq_sems, wo_sem, st_sems, ws_sems, c_sems, q_sems, o_sems, p_sems, g_sems, y_sems, h_sems, credit,
):
    here = Place()
    n_layers = cache_hbm.shape[0]
    d = x_buf.shape[1]
    rows = x_buf.shape[0]
    unit = c_buf.shape[1]
    units = rows // unit
    cols = w_buf.shape[2]
    chunk = stage.shape[1]
    heads = o_send.shape[2]
    kv = c_buf.shape[2]
    q_width = q_send.shape[-1] // 3
    chunks = len(CUBE_ORDERS)
    width = d // chunks
    swaps, h_copies = [], []
    partner = here.other(dc=1)
    peers = [here.other(dz=dz, dy=dy) for dz, dy in TP_PEERS]
    cube = [here.other(dx=dx, dz=dz, dy=dy) for dx, dz, dy in NEAR]

    def wq_copy(layer, n):
        part = slice(n * q_width, (n + 1) * q_width)
        return pltpu.make_async_copy(wq_hbm.at[layer, :, part], wq_buf.at[:, part], wq_sems.at[n])

    def wo_copy(layer):
        return pltpu.make_async_copy(wo_hbm.at[layer], wo_buf, wo_sem.at[0])

    def cache_copy(layer, i):
        slot = lax.rem(i, 2)
        return pltpu.make_async_copy(
            cache_hbm.at[layer, pl.ds(here.tp * rows + i * unit, unit)], c_buf.at[slot], c_sems.at[slot]
        )

    pieces = [
        (k, hbm, lo, min(chunk, cols - lo))
        for k, hbm in enumerate((w3_hbm, w1_hbm, w2_hbm)) for lo in range(0, cols, chunk)
    ]
    ring = stage.shape[0]

    def piece_copy(i):
        _, hbm, lo, n = pieces[i]
        return pltpu.make_async_copy(hbm.at[lo:lo + n], stage.at[i % ring, 0:n], st_sems.at[i % ring])

    def unpack(layer, i):
        k, _, lo, n = pieces[i]
        slot = i % ring

        @pl.loop(0, n // 16)
        def _(j):
            r = pl.multiple_of(j * 16, 16)
            pair = pltpu.einshape('alk->lak', stage[slot, pl.ds(r, 16)])
            w_buf[k, here.c, pl.ds(pl.multiple_of(lo + r, 16), 16), :] = pair[layer]
        if n % 16:
            r = n - n % 16
            pair = pltpu.einshape('alk->lak', stage[slot, r:n])
            w_buf[k, here.c, lo + r:lo + n, :] = pair[layer]

    def share(layer, i):
        piece_copy(i).wait()
        unpack(layer, i)
        if i + ring < len(pieces):
            piece_copy(i + ring).start()
        elif layer + 1 < n_layers:
            piece_copy(i + ring - len(pieces)).start()
        k = pieces[i][0]
        if i + 1 == len(pieces) or pieces[i + 1][0] != k:
            if layer and k == 0:
                pl.semaphore_wait(credit, 1)
            mine = w_buf.at[k, here.c]
            swaps.append(_send(mine, mine, ws_sems, k, partner))

    def exchange(src, dst, sems, i, k):
        return pltpu.make_async_remote_copy(
            src_ref=src.at[peers[k]['tp'], i], dst_ref=dst.at[here.tp, i],
            send_sem=sems.at[0, 3 * i + k], recv_sem=sems.at[1, 3 * i + k],
            device_id=peers[k], device_id_type=MESH,
        )

    q_copy = functools.partial(exchange, q_send, q_recv, q_sems)
    o_copy = functools.partial(exchange, o_send, o_all, o_sems)

    for n in range(3):
        wq_copy(0, n).start()
    for i in range(2):
        cache_copy(0, i).start()
    for i in range(ring):
        piece_copy(i).start()
    wo_copy(0).start()
    greeted = _greet(cube + [partner])

    for layer in range(n_layers):
        last = layer + 1 == n_layers
        x_all = x_ref if layer == 0 else h_all

        def h_norm(t):
            at = pl.multiple_of(t * rows, rows)
            h_buf[pl.ds(at, rows), :] = _norm(x_all[t], an_ref[layer:layer + 1, :])

        h_norm(here.tp)
        for k, peer in enumerate(peers):
            for copy in h_copies[k::3]:
                copy.wait_recv()
            h_norm(peer['tp'])
        for n in range(3):
            wq_copy(layer, n).wait()
            part = slice(n * q_width, (n + 1) * q_width)
            q = jnp.dot(h_buf[...], wq_buf[:, part], preferred_element_type=F32).astype(BF16)
            q_send[:, :, :, part] = q.reshape(4, units, unit, q_width)
        if layer == 0:
            greeted()
        for i in range(units):
            for k in range(3):
                q_copy(i, k).start()
        if not last:
            for n in range(3):
                wq_copy(layer + 1, n).start()
        q_recv[here.tp] = q_send[here.tp]

        if layer == 0:
            for i in range(len(pieces)):
                share(0, i)

        @pl.loop(0, units)
        def _(i):
            slot = lax.rem(i, 2)
            for k in range(3):
                q_copy(i, k).wait_recv()
            for h in range(heads):
                q = q_recv[:, i, :, h * kv:(h + 1) * kv]
                q_att[:, 4 * h:4 * h + 4, :] = pltpu.einshape('tbk->btk', q)
            cache_copy(layer, i).wait()
            for lo in range(0, unit, 4):
                scores = [
                    jnp.dot(q_att[k], c_buf[slot, k], preferred_element_type=F32)
                    for k in range(lo, lo + 4)
                ]
                probs = []
                for k, s in enumerate(scores, lo):
                    keep = lax.broadcasted_iota(jnp.int32, s.shape, 1) < len_ref[here.tp * rows + i * unit + k]
                    s = jnp.where(keep, s * SCALE, -jnp.inf)
                    e = jnp.exp(s - jnp.max(s, axis=-1, keepdims=True))
                    probs.append((e / jnp.sum(e, axis=-1, keepdims=True)).astype(BF16))
                for k, p in enumerate(probs, lo):
                    o = lax.dot_general(
                        p, c_buf[slot, k, 0:LAT, :], (((1,), (1,)), ((), ())), preferred_element_type=F32
                    )
                    for j in range(LAT // 128):
                        o_rows[j, k * 16:(k + 1) * 16, :] = o[:, j * 128:(j + 1) * 128]
            for h in range(heads):
                for t in range(4):
                    for j in range(LAT // 128):
                        part = slice(j * 128, (j + 1) * 128)
                        o_send[t, i, h, :, part] = o_rows[j, pl.ds(4 * h + t, unit, stride=16), :].astype(BF16)
            for k in range(3):
                o_copy(i, k).start()
            o_all[here.tp, i] = o_send[here.tp, i]

            @pl.when(i + 2 < units)
            def _():
                cache_copy(layer, i + 2).start()
        if not last:
            for i in range(2):
                cache_copy(layer + 1, i).start()
        wo_copy(layer).wait()
        for i in range(units):
            for k in range(3):
                o_copy(i, k).wait_recv()

        wide = p_buf.shape[-1]
        lhs = jnp.concatenate([o_all[:, :, h].reshape(4 * rows, LAT) for h in range(heads)], axis=1)
        attn = Halving(here, ('z', 'y'), p_buf, (pr1, pr2), p_sems, TP_ORDERS)
        for n in range(0, len(TP_ORDERS), 2):
            y = jnp.dot(lhs, wo_buf[:, n * wide:(n + 2) * wide], preferred_element_type=F32)
            for k in range(2):
                p_buf[n + k] = y[:, k * wide:(k + 1) * wide].reshape(p_buf.shape[1:])
                attn.send(n + k, 0)
        if not last:
            wo_copy(layer + 1).start()
        for n in range(len(TP_ORDERS)):
            attn.add(n, 0)
            attn.send(n, 1)
        x_mine = x_ref[here.tp] if layer == 0 else x_buf[...]
        g_copies = []

        def g_send(n, source, target, sem):
            device = here.other(*source)
            block = g_all.at[lax.div(device['dp'], 2), device['tp'], :, n * wide:(n + 1) * wide]
            return _send(block, block, g_sems, 7 * n + NEAR.index(sem), here.other(*target))

        for n in range(len(TP_ORDERS)):
            part = slice(n * wide, (n + 1) * wide)
            total = attn.add(n, 1).astype(BF16)
            x_part = (x_mine[:, part].astype(F32) + total.astype(F32)).astype(BF16)
            x_buf[:, part] = x_part
            g_all[here.x, here.tp, :, part] = x_part
            axis = CROSSINGS[n]
            sent = {}
            for offset in NEAR:
                if offset == axis or not _meet(offset, axis):
                    sent[offset] = g_send(n, (0, 0, 0), offset, offset)
            g_copies.append(sent)
        for n, sent in enumerate(g_copies):
            axis = CROSSINGS[n]
            for offset in NEAR:
                if not _meet(offset, axis):
                    sent[offset].wait_recv()
                    both = tuple(a + b for a, b in zip(offset, axis))
                    sent[both] = g_send(n, offset, axis, both)

        def g_norm(x, t):
            at = pl.multiple_of((4 * x + t) * rows, rows)
            g_buf[pl.ds(at, rows), :] = _norm(g_all[x, t], fn_ref[layer:layer + 1, :])

        g_norm(here.x, here.tp)
        for copy in swaps:
            copy.wait()
        swaps.clear()
        for offset, device in zip(NEAR, cube):
            for n, sent in enumerate(g_copies):
                if _meet(offset, CROSSINGS[n]):
                    sent[offset].wait_recv()
            g_norm(lax.div(device['dp'], 2), device['tp'])

        for sent in g_copies:
            for copy in sent.values():
                copy.wait_send()

        @pl.loop(0, 2)
        def _(s):
            for lo in range(0, cols, 256):
                part = slice(lo, min(lo + 256, cols))
                u, v = (
                    lax.dot_general(
                        w_buf[k, s, part, :], g_buf[...], (((1,), (1,)), ((), ())), preferred_element_type=F32
                    ) for k in range(2)
                )
                a_buf[s, :, part] = (u * jax.nn.sigmoid(u) * v).T.astype(BF16)

        ffn = Halving(here, ('x', 'z', 'y'), y_buf, (yr1, yr2, yr3), y_sems, CUBE_ORDERS)
        for n in range(chunks):
            part = slice(n * width, (n + 1) * width)
            y = jnp.dot(a_buf[0], w_buf[2, 0, :, part], preferred_element_type=F32)
            y += jnp.dot(a_buf[1], w_buf[2, 1, :, part], preferred_element_type=F32)
            y_buf[n] = y.reshape(y_buf.shape[1:])
            ffn.send(n, 0)
        if not last:
            pl.semaphore_signal(credit, inc=1, device_id=partner, device_id_type=MESH)
        for phase in range(2):
            for n in range(chunks):
                ffn.add(n, phase)
                ffn.send(n, phase + 1)
                if not last and phase * chunks + n < len(pieces):
                    share(layer + 1, phase * chunks + n)
        h_copies = []
        for n in range(chunks):
            part = slice(n * width, (n + 1) * width)
            total = ffn.add(n, 2).astype(BF16)
            x_part = (x_buf[:, part].astype(F32) + total.astype(F32)).astype(BF16)
            x_buf[:, part] = x_part
            h_all[here.tp, :, part] = x_part
            mine = h_all.at[here.tp, :, part]
            h_copies += [_send(mine, mine, h_sems, 3 * n + k, peer) for k, peer in enumerate(peers)]

        attn.finish()
        ffn.finish()
        for copy in h_copies:
            copy.wait_send()
        for i in range(units):
            for k in range(3):
                q_copy(i, k).wait_send()
                o_copy(i, k).wait_send()
    for copy in h_copies:
        copy.wait_recv()
    out_ref[...] = h_all[...]


VM = pl.BlockSpec(memory_space=pltpu.VMEM)
SM = pl.BlockSpec(memory_space=pltpu.SMEM)
ANY = pl.BlockSpec(memory_space=pl.ANY)
DMA = pltpu.SemaphoreType.DMA


def solution(mesh):
    def body(x, lengths, cache, attn_norm, ffn_norm, wq, wo, w1, w3, w2):
        nb, d = x.shape
        s_len, kv = cache.shape[2:]
        heads = wq.shape[2] // kv
        rows = nb // 4
        cols = w1.shape[2]
        unit = 8
        q_shape = (4, rows // unit, unit, heads * kv)
        scratch = [
            pltpu.VMEM(wq.shape[1:], BF16),
            pltpu.VMEM(wo.shape[1:], BF16),
            pltpu.VMEM((3, 2, cols, d), BF16),
            pltpu.VMEM((2, 176, 2, d), BF16),
            pltpu.VMEM((2, unit, kv, s_len), BF16),
            pltpu.VMEM((nb, d), BF16),
            pltpu.VMEM(q_shape, BF16),
            pltpu.VMEM(q_shape, BF16),
            pltpu.VMEM((unit, 4 * heads, kv), BF16),
            pltpu.VMEM((LAT // 128, unit * 4 * heads, 128), F32),
            pltpu.VMEM((4, rows // unit, heads, unit, LAT), BF16),
            pltpu.VMEM((4, rows // unit, heads, unit, LAT), BF16),
            pltpu.VMEM((8, 2, 2, rows, d // 8), F32),
            pltpu.VMEM((8, 2, rows, d // 8), F32),
            pltpu.VMEM((8, rows, d // 8), F32),
            pltpu.VMEM((rows, d), BF16),
            pltpu.VMEM((2, 4, rows, d), BF16),
            pltpu.VMEM((8 * rows, d), BF16),
            pltpu.VMEM((2, 8 * rows, cols), BF16),
            pltpu.VMEM((8, 2, 2, 2, rows, d // 8), F32),
            pltpu.VMEM((8, 2, 2, rows, d // 8), F32),
            pltpu.VMEM((8, 2, rows, d // 8), F32),
            pltpu.VMEM((8, rows, d // 8), F32),
            pltpu.VMEM((4, rows, d), BF16),
            DMA((3,)),
            DMA((1,)),
            DMA((2,)),
            DMA((2, 3)),
            DMA((2,)),
            DMA((2, 12)),
            DMA((2, 12)),
            DMA((2, 16)),
            DMA((2, 56)),
            DMA((2, 24)),
            DMA((2, 24)),
            pltpu.SemaphoreType.REGULAR,
        ]
        out = pl.pallas_call(
            _kernel,
            out_shape=jax.ShapeDtypeStruct((4, rows, d), BF16),
            in_specs=[SM, VM, VM, VM] + [ANY] * 6,
            out_specs=VM,
            scratch_shapes=scratch,
            compiler_params=pltpu.CompilerParams(
                collective_id=0, has_side_effects=True, vmem_limit_bytes=VMEM_LIMIT,
            ),
            name='two_layers',
        )(
            lengths, x.reshape(4, rows, d), attn_norm, ffn_norm, cache.transpose(0, 1, 3, 2), wq, wo,
            w1.transpose(2, 0, 1), w3.transpose(2, 0, 1), w2.transpose(1, 0, 2),
        )
        return out.reshape(nb, d)

    in_specs = (
        P('dp', None),
        P('dp'),
        P(None, 'dp', None, None),
        P(None, None),
        P(None, None),
        P(None, None, 'tp'),
        P(None, 'tp', None),
        P(None, None, ('dp', 'tp')),
        P(None, None, ('dp', 'tp')),
        P(None, ('dp', 'tp'), None),
    )
    return jax.shard_map(body, mesh=mesh, in_specs=in_specs, out_specs=P('dp', None), check_vma=False)
```
